256 devices in a mesh: blk: 4 (over x), grp: 64 (over z, y, core).
Axes of the slice: x: 4, y: 4, z: 8, core: 2. Of those that a mesh axis runs over, the one named last changes fastest.
Arguments:
- points: float32 [3, 32768], P(None, ('blk', 'grp')), may hold values from 0 to 1
- labels: int32 [32768], P(('blk', 'grp')), may hold values 0 or 1
- shape_scale: float32 [32768], P(('blk', 'grp')), may hold values from 0.1 to 0.4
- krylov_basis: float32 [8, 32, 32768], P(None, None, ('blk', 'grp')), may hold values from -6 to 6
- sketch: float32 [1024, 32768], P(None, ('blk', 'grp')), may hold values from -0.03125 to 0.03125
- sketched_basis: float32 [8, 32, 1024], replicated, may hold values from -0.1875 to 0.1875
Outputs:
- next_vector: float32 [32, 32768], P(None, ('blk', 'grp'))
- coefficients: float32 [8, 32], replicated
- sketch_next: float32 [32, 1024], replicated
- norms: float32 [32], replicated
The draws below stay inside these ranges and needn't reach their ends.
All inputs are finite; a program needn't handle non-finite values. No bound on the sum of `labels` on one device may be relied on, other than what follows from the above.
Results may differ from the reference program's by a relative error of at most 0.0003.
Values sent between devices are 32-bit elements; how exact they have to be, the bound alone decides.
No kernel may reach another device: no remote copies, remote signals or barrier semaphores. Data moves between devices by JAX's collectives and lax.ppermute only.
A program may use at most 64 MiB of HBM per device.

```python
import math
import jax
import jax.numpy as jnp
from jax import lax

SYSTEMS = 32
KRYLOV = 8
SKETCH = 1024
N = 32768


def draw_points(key, part):
    first_key = jax.random.fold_in(key, 11)
    second_key = jax.random.fold_in(key, 12)
    third_key = jax.random.fold_in(key, 13)
    across = jax.random.uniform(first_key, (N,), jnp.float32)
    depth = jax.random.uniform(second_key, (N,), jnp.float32)
    jitter = jax.random.uniform(third_key, (N,), jnp.float32)
    ordering = jnp.arange(N).astype(jnp.float32)
    height = (ordering + jitter) / N
    return jnp.stack([across, depth, height], axis=0).astype(jnp.float32)


def place_ends(drawn, key, smallest, top_value):
    place = [jax.random.randint(jax.random.fold_in(key, axis), (), 0, length) for axis, length in enumerate(drawn.shape)]
    widest = drawn.shape.index(max(drawn.shape))
    neighbour = place[:widest] + [(place[widest] + 1) % drawn.shape[widest]] + place[widest + 1:]
    return drawn.at[tuple(place)].set(smallest).at[tuple(neighbour)].set(top_value)


def block_levels(rng, dims, split, smallest, largest):
    def one(position, shards_of):
        draws = jax.random.uniform(jax.random.fold_in(jax.random.fold_in(rng, 6), position), (shards_of,), jnp.float32, smallest / len(split), largest / len(split))
        return jnp.repeat(jnp.exp(draws), dims[position] // shards_of).reshape((-1,) + (1,) * (len(dims) - position - 1))

    factor_of = one(*split[0])
    for cut in split[1:]:
        factor_of = factor_of * one(*cut)
    return factor_of


def gaussian(key, shape, width, bound, cuts=(), held_as=jnp.bfloat16):
    values = width * jax.random.normal(key, shape, jnp.float32)
    if cuts:
        values = values * block_levels(key, shape, cuts, -0.22, 0.18)
    return jnp.clip(values, -bound, bound).astype(held_as)


def setup_inputs(seed: int = 0) -> dict:
    key_list = jax.random.split(jax.random.key(seed), 7)
    points = draw_points(jax.random.fold_in(key_list[6], 71), 0)
    labels = place_ends((jax.random.randint(key_list[1], (N,), 0, 4) < 3).astype(jnp.int32), jax.random.fold_in(key_list[1], 1), 0, 1)
    shape_scale = jnp.clip(jnp.exp(math.log(0.4) - 1.3862944 * jax.random.uniform(key_list[2], (N,), jnp.float32) ** block_levels(key_list[2], (N,), ((0, 256),), -0.2, 0.2)), 0.1, 0.4)
    krylov_basis = gaussian(key_list[3], (KRYLOV, SYSTEMS, N), 1.0, 6.0, ((2, 256),), jnp.float32)
    sketch = gaussian(key_list[4], (SKETCH, N), N ** -0.5, 0.03125, ((1, 256),), jnp.float32)
    sketched_basis = gaussian(key_list[5], (KRYLOV, SYSTEMS, SKETCH), SKETCH ** -0.5, 0.1875, (), jnp.float32)
    return dict(points=points, labels=labels, shape_scale=shape_scale, krylov_basis=krylov_basis, sketch=sketch, sketched_basis=sketched_basis)


def kernel_terms(target_points, target_labels, source_block):
    source_points = source_block[0:3]
    scales = source_block[3]
    weights_block = source_block[4:]
    delta_x = source_points[0][:, None] - target_points[0][None, :]
    delta_y = source_points[1][:, None] - target_points[1][None, :]
    delta_z = source_points[2][:, None] - target_points[2][None, :]
    radius_sq = delta_x * delta_x + delta_y * delta_y + delta_z * delta_z
    squared_scale = (scales * scales)[:, None]
    shifted = radius_sq + squared_scale
    inverse = lax.rsqrt(shifted)
    boundary = shifted * inverse
    interior = (3.0 * squared_scale + 2.0 * radius_sq) * inverse * inverse * inverse
    kernel = jnp.where(target_labels[None, :] == 1, interior, boundary)
    return jnp.dot(weights_block, kernel, precision=lax.Precision.HIGHEST, preferred_element_type=jnp.float32)

def block_size(length, wanted):
    return wanted if length % wanted == 0 else length

def reference(points, labels, shape_scale, krylov_basis, sketch, sketched_basis):
    sources = jnp.concatenate([points, shape_scale[None, :], krylov_basis[KRYLOV - 1]], axis=0)
    width_rows = sources.shape[0]
    tblock = block_size(N, 2048)
    sblock = block_size(N, 2048)
    source_blocks = jnp.transpose(sources.reshape(width_rows, N // sblock, sblock), (1, 0, 2))
    target_blocks = jnp.transpose(points.reshape(3, N // tblock, tblock), (1, 0, 2))
    label_blocks = labels.reshape(N // tblock, tblock)

    def one_target(packed):
        target_points, target_labels = packed

        def over_sources(running, block):
            return (running + kernel_terms(target_points, target_labels, block), None)
        start_value = jnp.zeros((SYSTEMS, tblock), jnp.float32)
        result, unused = lax.scan(over_sources, start_value, source_blocks)
        return result
    pieces = lax.map(one_target, (target_blocks, label_blocks))
    image = jnp.transpose(pieces, (1, 0, 2)).reshape(SYSTEMS, N) / jnp.sqrt(jnp.float32(N))
    sketched = lax.dot_general(image, sketch, (((1,), (1,)), ((), ())), precision=lax.Precision.HIGHEST, preferred_element_type=jnp.float32)
    coefficients = jnp.einsum('jrk,rk->jr', sketched_basis, sketched, precision=lax.Precision.HIGHEST)
    remainder = sketched - jnp.einsum('jr,jrk->rk', coefficients, sketched_basis, precision=lax.Precision.HIGHEST)
    norms = jnp.sqrt(lax.optimization_barrier(jnp.mean(remainder * remainder, axis=1)) + 1e-06)
    sketch_next = remainder / norms[:, None]
    reduced = image - jnp.einsum('jr,jrn->rn', coefficients, krylov_basis, precision=lax.Precision.HIGHEST)
    next_vector = reduced / norms[:, None]
    return (next_vector, coefficients, sketch_next, norms)
```

```python
import functools
import math

import jax
import jax.numpy as jnp
from jax import lax
from jax.experimental import pallas as pl
from jax.experimental.pallas import tpu as pltpu
from jax.sharding import Mesh
from jax.sharding import PartitionSpec as P

SYSTEMS = 32
KRYLOV = 8
FEATS = 32
LANES = 128
ALL = ("blk", "grp_0", "grp_1", "grp_2")
ROW = ("blk", "grp_1")
COLUMN = ("grp_0", "grp_2")
OWNERS = ("blk", "grp_1", "grp_2")
VMEM = pl.BlockSpec(memory_space=pltpu.VMEM)
MIB = 2**20


def exchange(value, axis):
    return lax.all_to_all(value, axis, 0, 0, tiled=True)


def copies(value, axis):
    return jnp.broadcast_to(value[None], (lax.axis_size(axis), *value.shape))


def parts(value):
    first = value.astype(jnp.bfloat16).astype(jnp.float32)
    rest = value - first
    second = rest.astype(jnp.bfloat16).astype(jnp.float32)
    return [first, second, rest - second]


def wide(tiles):
    return jnp.concatenate(tiles, axis=1)


def pair_kernel(tblock, sblock, source_ref, target_ref, out_ref, source_feats, target_feats, squares, weights):
    blocks, owners = source_ref.shape[0], target_ref.shape[0]
    zero = jnp.zeros((blocks, LANES), jnp.float32)
    one = zero + 1.0
    coords = [source_ref[:, SYSTEMS + a, :] - 0.5 for a in range(3)]
    scale = source_ref[:, SYSTEMS + 3, :]
    scale_sq = scale * scale
    rows = []
    for value in coords:
        a, b, c = parts(value)
        rows += [a, a, b, b, a, c]
    rows += parts(coords[0] * coords[0] + coords[1] * coords[1] + coords[2] * coords[2] + scale_sq)
    rows += [one] * 3 + parts(scale_sq)
    rows += [zero] * (FEATS - len(rows))
    for k, value in enumerate(rows):
        source_feats[:, k, :] = value
    zero = jnp.zeros((owners, LANES), jnp.float32)
    one = zero + 1.0
    coords = [target_ref[:, a, :] - 0.5 for a in range(3)]
    rows = []
    for value in coords:
        a, b, c = parts(-2.0 * value)
        rows += [a, b, a, b, c, a]
    rows += [one] * 3
    rows += parts(coords[0] * coords[0] + coords[1] * coords[1] + coords[2] * coords[2])
    rows += [zero] * (FEATS - len(rows))
    for k, value in enumerate(rows):
        target_feats[:, k, :] = value
    row = lax.broadcasted_iota(jnp.int32, (FEATS, LANES), 0)
    pick = jnp.where(jnp.logical_and(row >= 24, row < 27), 1.0, 0.0).astype(jnp.bfloat16)
    steps, per, tper = blocks * LANES // sblock, sblock // LANES, tblock // LANES
    over_rows = (((0,), (0,)), ((), ()))

    def feats_of(step):
        return wide([source_feats[step * per + j] for j in range(per)]).astype(jnp.bfloat16)

    for step in range(steps):
        squares[step * sblock : (step + 1) * sblock, :] = lax.dot_general(
            feats_of(step), pick, over_rows, preferred_element_type=jnp.float32
        )
        weight = wide([source_ref[step * per + j, 0:SYSTEMS, :] for j in range(per)])
        first = weight.astype(jnp.bfloat16)
        second = (weight - first.astype(jnp.float32)).astype(jnp.bfloat16)
        weights[step] = jnp.concatenate([first, second], axis=0)

    def over_targets(index, carry):
        feats = wide([target_feats[index * tper + j] for j in range(tper)]).astype(jnp.bfloat16)
        inner = wide([target_ref[index * tper + j, 3:4, :] for j in range(tper)]) > 0.5
        total = jnp.zeros((2 * SYSTEMS, tblock), jnp.float32)
        for step in range(steps):
            shifted = lax.dot_general(
                feats_of(step), feats, over_rows, preferred_element_type=jnp.float32
            )
            inverse = lax.rsqrt(shifted)
            square = wide([squares[step * sblock : (step + 1) * sblock, :]] * tper)
            kernel = inverse * jnp.where(inner, 2.0 + square * (inverse * inverse), shifted)
            first = kernel.astype(jnp.bfloat16)
            second = (kernel - first.astype(jnp.float32)).astype(jnp.bfloat16)
            weight = weights[step]
            total = (
                total
                + jnp.dot(weight, first, preferred_element_type=jnp.float32)
                + jnp.dot(weight, second, preferred_element_type=jnp.float32)
            )
        result = total[:SYSTEMS] + total[SYSTEMS:]
        for j in range(tper):
            out_ref[index * tper + j] = result[:, j * LANES : (j + 1) * LANES]
        return carry

    lax.fori_loop(0, owners // tper, over_targets, 0)


def pair_product(sources, targets, tblock=256, sblock=128):
    blocks, owners = sources.shape[0], targets.shape[0]
    pairs = blocks * owners * LANES * LANES
    return pl.pallas_call(
        functools.partial(pair_kernel, tblock, sblock),
        out_shape=jax.ShapeDtypeStruct((owners, SYSTEMS, LANES), jnp.float32),
        in_specs=[VMEM] * 2,
        out_specs=VMEM,
        scratch_shapes=[
            pltpu.VMEM((blocks, FEATS, LANES), jnp.float32),
            pltpu.VMEM((owners, FEATS, LANES), jnp.float32),
            pltpu.VMEM((blocks * LANES, LANES), jnp.float32),
            pltpu.VMEM((blocks * LANES // sblock, 2 * SYSTEMS, sblock), jnp.bfloat16),
        ],
        cost_estimate=pl.CostEstimate(flops=6 * SYSTEMS * pairs, bytes_accessed=2**20, transcendentals=pairs),
        name="pairs",
        compiler_params=pltpu.CompilerParams(vmem_limit_bytes=16 * MIB),
    )(sources, targets)


def image_kernel(root, arrived_ref, sketch_ref, image_ref, local_ref):
    total = arrived_ref[0]
    for k in range(1, arrived_ref.shape[0]):
        total = total + arrived_ref[k]
    image = total / root
    image_ref[...] = image
    for k in range(sketch_ref.shape[0] // LANES):
        local_ref[:, k, :] = lax.dot_general(
            image,
            sketch_ref[k * LANES : (k + 1) * LANES, :],
            (((1,), (1,)), ((), ())),
            precision=lax.Precision.HIGHEST,
            preferred_element_type=jnp.float32,
        )


def image_and_sketch(arrived, sketch, root):
    rows = sketch.shape[0]
    return pl.pallas_call(
        functools.partial(image_kernel, root),
        out_shape=(
            jax.ShapeDtypeStruct((SYSTEMS, LANES), jnp.float32),
            jax.ShapeDtypeStruct((SYSTEMS, rows // LANES, LANES), jnp.float32),
        ),
        in_specs=[VMEM] * 2,
        out_specs=(VMEM,) * 2,
        name="image",
        compiler_params=pltpu.CompilerParams(vmem_limit_bytes=8 * MIB),
    )(arrived, sketch)


def sum_kernel(arrived_ref, out_ref):
    total = arrived_ref[0]
    for k in range(1, arrived_ref.shape[0]):
        total = total + arrived_ref[k]
    for k in range(out_ref.shape[0]):
        out_ref[k] = total


def sum_for_each(arrived, count):
    return pl.pallas_call(
        sum_kernel,
        out_shape=jax.ShapeDtypeStruct((count, *arrived.shape[1:]), jnp.float32),
        in_specs=[VMEM],
        out_specs=VMEM,
        name="addup",
        compiler_params=pltpu.CompilerParams(vmem_limit_bytes=4 * MIB),
    )(arrived)


def project_kernel(arrived_ref, basis_ref, out_ref):
    sketched = arrived_ref[0]
    for k in range(1, arrived_ref.shape[0]):
        sketched = sketched + arrived_ref[k]
    lane = lax.broadcasted_iota(jnp.int32, (8, LANES), 1)

    def whole(value):
        return jnp.sum(jnp.sum(value, axis=1, keepdims=True), axis=0, keepdims=True)

    scalars = jnp.zeros((8, LANES), jnp.float32)
    remainder = sketched
    for j in range(KRYLOV):
        coefficient = whole(basis_ref[j] * sketched)
        scalars = jnp.where(lane == j, coefficient, scalars)
        remainder = remainder - coefficient * basis_ref[j]
    norm = jnp.sqrt(whole(remainder * remainder) / (sketched.shape[0] * LANES) + 1e-06)
    scalars = jnp.where(lane == KRYLOV, norm, scalars)
    message = jnp.concatenate([remainder / norm, scalars], axis=0)
    for k in range(out_ref.shape[0]):
        out_ref[k] = message


def project(arrived, basis, count):
    return pl.pallas_call(
        project_kernel,
        out_shape=jax.ShapeDtypeStruct((count, arrived.shape[1] + 8, LANES), jnp.float32),
        in_specs=[VMEM] * 2,
        out_specs=VMEM,
        name="project",
        compiler_params=pltpu.CompilerParams(vmem_limit_bytes=4 * MIB),
    )(arrived, basis)


def finish_kernel(arrived_ref, image_ref, krylov_ref, next_ref, coefficients_ref, sketch_ref, norms_ref):
    rows = arrived_ref.shape[1] - 8
    for k in range(rows):
        sketch_ref[:, k * LANES : (k + 1) * LANES] = arrived_ref[:, k, :]
    scalars = arrived_ref[:, rows, :]
    reduced = image_ref[...]
    for j in range(KRYLOV):
        reduced = reduced - scalars[:, j : j + 1] * krylov_ref[j]
    next_ref[...] = reduced / scalars[:, KRYLOV : KRYLOV + 1]
    across = jnp.transpose(scalars)
    coefficients_ref[...] = across[0:KRYLOV, :]
    norms_ref[...] = across[KRYLOV : KRYLOV + 1, :]


def finish(arrived, image, krylov):
    rows = arrived.shape[1] - 8
    return pl.pallas_call(
        finish_kernel,
        out_shape=(
            jax.ShapeDtypeStruct((SYSTEMS, LANES), jnp.float32),
            jax.ShapeDtypeStruct((KRYLOV, SYSTEMS), jnp.float32),
            jax.ShapeDtypeStruct((SYSTEMS, rows * LANES), jnp.float32),
            jax.ShapeDtypeStruct((1, SYSTEMS), jnp.float32),
        ),
        in_specs=[VMEM] * 3,
        out_specs=(VMEM,) * 4,
        name="finish",
        compiler_params=pltpu.CompilerParams(vmem_limit_bytes=8 * MIB),
    )(arrived, image, krylov)


def shards(points, labels, shape_scale, krylov_basis, sketch, sketched_basis):
    everything = lax.axis_size(ALL) * points.shape[1]
    sources = jnp.concatenate([krylov_basis[KRYLOV - 1], points, shape_scale[None, :]], axis=0)
    targets = jnp.concatenate([points, labels[None, :].astype(jnp.float32)], axis=0)
    system = lax.axis_index(OWNERS)
    basis = lax.dynamic_slice_in_dim(sketched_basis, system, 1, axis=1)
    basis = basis.reshape(KRYLOV, -1, LANES)
    all_targets = exchange(copies(targets, COLUMN), COLUMN)
    all_sources = exchange(copies(sources, ROW), ROW)
    partial_value = pair_product(all_sources, all_targets)
    image, local_sketch = image_and_sketch(
        exchange(partial_value, COLUMN), sketch, math.sqrt(everything)
    )
    over_owners = sum_for_each(exchange(local_sketch, OWNERS), lax.axis_size("grp_0"))
    message = project(exchange(over_owners, "grp_0"), basis, lax.axis_size(OWNERS))
    next_vector, coefficients, sketch_next, norms = finish(
        exchange(message, OWNERS), image, krylov_basis
    )
    return (next_vector, coefficients, sketch_next, norms.reshape(-1))


def solution(mesh):
    torus = Mesh(mesh.devices.reshape(mesh.shape["blk"], 8, 4, 2), ALL)
    in_specs = (P(None, ALL), P(ALL), P(ALL), P(None, None, ALL), P(None, ALL), P())
    out_specs = (P(None, ALL), P(), P(), P())
    return jax.shard_map(
        shards, mesh=torus, in_specs=in_specs, out_specs=out_specs, check_vma=False
    )
```

```python
import functools
import math

import jax
import jax.numpy as jnp
from jax import lax
from jax.experimental import pallas as pl
from jax.experimental.pallas import tpu as pltpu
from jax.sharding import Mesh
from jax.sharding import PartitionSpec as P

SYSTEMS = 32
KRYLOV = 8
FEATS = 32
LANES = 128
X1, X0, Z2, Z1, Z0, Y1, Y0, CORE = ALL = ("x1", "x0", "z2", "z1", "z0", "y1", "y0", "core")
COLUMN = (X0, Y1, Y0, CORE)
ROW = (X1, Z2, Z1, Z0)
OWNERS = (X1, X0, Y1, Y0, CORE)
LAYERS = (Z2, Z1, Z0)
VMEM = pl.BlockSpec(memory_space=pltpu.VMEM)
MIB = 2**20


def exchange(value, axis):
    return lax.all_to_all(value, axis, 0, 0, tiled=True)


def gather_by_distance(value, axes):
    for axis in reversed(axes):
        value = jnp.concatenate([value, lax.ppermute(value, axis, ((0, 1), (1, 0)))], axis=0)
    return value


def parts(value):
    first = value.astype(jnp.bfloat16).astype(jnp.float32)
    rest = value - first
    second = rest.astype(jnp.bfloat16).astype(jnp.float32)
    return [first, second, rest - second]


def wide(tiles):
    return jnp.concatenate(tiles, axis=1)


def message_kernel(points_ref, labels_ref, scale_ref, vector_ref, sources_ref, targets_ref):
    for k in range(sources_ref.shape[0]):
        sources_ref[k, 0:SYSTEMS, :] = vector_ref[0]
        sources_ref[k, SYSTEMS : SYSTEMS + 3, :] = points_ref[...]
        sources_ref[k, SYSTEMS + 3 : SYSTEMS + 4, :] = scale_ref[...]
    targets_ref[0, 0:3, :] = points_ref[...]
    targets_ref[0, 3:4, :] = labels_ref[...].astype(jnp.float32)


def messages(points, labels, shape_scale, krylov, count):
    last = krylov.shape[0] - 1
    whole = lambda shape: pl.BlockSpec(shape, lambda i: (0,) * len(shape))
    return pl.pallas_call(
        message_kernel,
        grid=(1,),
        out_shape=(
            jax.ShapeDtypeStruct((count, SYSTEMS + 4, LANES), jnp.float32),
            jax.ShapeDtypeStruct((1, 4, LANES), jnp.float32),
        ),
        in_specs=[
            whole((3, LANES)),
            whole((1, LANES)),
            whole((1, LANES)),
            pl.BlockSpec((1, SYSTEMS, LANES), lambda i: (last, 0, 0)),
        ],
        out_specs=(whole((count, SYSTEMS + 4, LANES)), whole((1, 4, LANES))),
        name="messages",
        compiler_params=pltpu.CompilerParams(vmem_limit_bytes=4 * MIB),
    )(points, labels[None, :], shape_scale[None, :], krylov)


def pair_kernel(tblock, sblock, source_ref, target_ref, out_ref, source_feats, target_feats, squares, weights):
    blocks, owners = source_ref.shape[0], target_ref.shape[0]
    zero = jnp.zeros((blocks, LANES), jnp.float32)
    one = zero + 1.0
    coords = [source_ref[:, SYSTEMS + a, :] - 0.5 for a in range(3)]
    scale = source_ref[:, SYSTEMS + 3, :]
    scale_sq = scale * scale
    rows = []
    for value in coords:
        a, b, c = parts(value)
        rows += [a, a, b, b, a, c]
    rows += parts(coords[0] * coords[0] + coords[1] * coords[1] + coords[2] * coords[2] + scale_sq)
    rows += [one] * 3 + parts(scale_sq)
    rows += [zero] * (FEATS - len(rows))
    for k, value in enumerate(rows):
        source_feats[:, k, :] = value
    zero = jnp.zeros((owners, LANES), jnp.float32)
    one = zero + 1.0
    coords = [target_ref[:, a, :] - 0.5 for a in range(3)]
    rows = []
    for value in coords:
        a, b, c = parts(-2.0 * value)
        rows += [a, b, a, b, c, a]
    rows += [one] * 3
    rows += parts(coords[0] * coords[0] + coords[1] * coords[1] + coords[2] * coords[2])
    rows += [zero] * (FEATS - len(rows))
    for k, value in enumerate(rows):
        target_feats[:, k, :] = value
    place = lax.axis_index(COLUMN)
    row = lax.broadcasted_iota(jnp.int32, (FEATS, LANES), 0)
    pick = jnp.where(jnp.logical_and(row >= 24, row < 27), 1.0, 0.0).astype(jnp.bfloat16)
    steps, per, tper = blocks * LANES // sblock, sblock // LANES, tblock // LANES
    over_rows = (((0,), (0,)), ((), ()))

    def feats_of(step):
        return wide([source_feats[step * per + j] for j in range(per)]).astype(jnp.bfloat16)

    for step in range(steps):
        squares[step * sblock : (step + 1) * sblock, :] = lax.dot_general(
            feats_of(step), pick, over_rows, preferred_element_type=jnp.float32
        )
        weight = wide([source_ref[step * per + j, 0:SYSTEMS, :] for j in range(per)])
        first = weight.astype(jnp.bfloat16)
        second = (weight - first.astype(jnp.float32)).astype(jnp.bfloat16)
        weights[step] = jnp.concatenate([first, second], axis=0)

    def over_targets(index, carry):
        feats = wide([target_feats[index * tper + j] for j in range(tper)]).astype(jnp.bfloat16)
        inner = wide([target_ref[index * tper + j, 3:4, :] for j in range(tper)]) > 0.5
        total = jnp.zeros((2 * SYSTEMS, tblock), jnp.float32)
        for step in range(steps):
            shifted = lax.dot_general(
                feats_of(step), feats, over_rows, preferred_element_type=jnp.float32
            )
            inverse = lax.rsqrt(shifted)
            square = wide([squares[step * sblock : (step + 1) * sblock, :]] * tper)
            kernel = inverse * jnp.where(inner, 2.0 + square * (inverse * inverse), shifted)
            first = kernel.astype(jnp.bfloat16)
            second = (kernel - first.astype(jnp.float32)).astype(jnp.bfloat16)
            weight = weights[step]
            total = (
                total
                + jnp.dot(weight, first, preferred_element_type=jnp.float32)
                + jnp.dot(weight, second, preferred_element_type=jnp.float32)
            )
        result = total[:SYSTEMS] + total[SYSTEMS:]
        for j in range(tper):
            out_ref[jnp.bitwise_xor(place, index * tper + j)] = result[:, j * LANES : (j + 1) * LANES]
        return carry

    lax.fori_loop(0, owners // tper, over_targets, 0)


def pair_product(sources, targets, tblock=256, sblock=128):
    blocks, owners = sources.shape[0], targets.shape[0]
    pairs = blocks * owners * LANES * LANES
    return pl.pallas_call(
        functools.partial(pair_kernel, tblock, sblock),
        out_shape=jax.ShapeDtypeStruct((owners, SYSTEMS, LANES), jnp.float32),
        in_specs=[VMEM] * 2,
        out_specs=VMEM,
        scratch_shapes=[
            pltpu.VMEM((blocks, FEATS, LANES), jnp.float32),
            pltpu.VMEM((owners, FEATS, LANES), jnp.float32),
            pltpu.VMEM((blocks * LANES, LANES), jnp.float32),
            pltpu.VMEM((blocks * LANES // sblock, 2 * SYSTEMS, sblock), jnp.bfloat16),
        ],
        cost_estimate=pl.CostEstimate(flops=6 * SYSTEMS * pairs, bytes_accessed=2**20, transcendentals=pairs),
        name="pairs",
        compiler_params=pltpu.CompilerParams(vmem_limit_bytes=16 * MIB),
    )(sources, targets)


def image_kernel(root, arrived_ref, sketch_ref, image_ref, local_ref):
    total = arrived_ref[0]
    for k in range(1, arrived_ref.shape[0]):
        total = total + arrived_ref[k]
    image = total / root
    image_ref[...] = image
    for k in range(sketch_ref.shape[0] // LANES):
        local_ref[:, k, :] = lax.dot_general(
            image,
            sketch_ref[k * LANES : (k + 1) * LANES, :],
            (((1,), (1,)), ((), ())),
            precision=lax.Precision.HIGHEST,
            preferred_element_type=jnp.float32,
        )


def image_and_sketch(arrived, sketch, root):
    rows = sketch.shape[0]
    return pl.pallas_call(
        functools.partial(image_kernel, root),
        out_shape=(
            jax.ShapeDtypeStruct((SYSTEMS, LANES), jnp.float32),
            jax.ShapeDtypeStruct((SYSTEMS, rows // LANES, LANES), jnp.float32),
        ),
        in_specs=[VMEM] * 2,
        out_specs=(VMEM,) * 2,
        name="image",
        compiler_params=pltpu.CompilerParams(vmem_limit_bytes=8 * MIB),
    )(arrived, sketch)


def sum_kernel(arrived_ref, out_ref):
    total = arrived_ref[0]
    for k in range(1, arrived_ref.shape[0]):
        total = total + arrived_ref[k]
    for k in range(out_ref.shape[0]):
        out_ref[k] = total


def sum_for_each(arrived, count):
    return pl.pallas_call(
        sum_kernel,
        out_shape=jax.ShapeDtypeStruct((count, *arrived.shape[1:]), jnp.float32),
        in_specs=[VMEM],
        out_specs=VMEM,
        name="addup",
        compiler_params=pltpu.CompilerParams(vmem_limit_bytes=4 * MIB),
    )(arrived)


def project_kernel(arrived_ref, basis_ref, out_ref):
    sketched = arrived_ref[0]
    for k in range(1, arrived_ref.shape[0]):
        sketched = sketched + arrived_ref[k]
    lane = lax.broadcasted_iota(jnp.int32, (8, LANES), 1)

    def whole(value):
        return jnp.sum(jnp.sum(value, axis=1, keepdims=True), axis=0, keepdims=True)

    scalars = jnp.zeros((8, LANES), jnp.float32)
    remainder = sketched
    for j in range(KRYLOV):
        coefficient = whole(basis_ref[j] * sketched)
        scalars = jnp.where(lane == j, coefficient, scalars)
        remainder = remainder - coefficient * basis_ref[j]
    norm = jnp.sqrt(whole(remainder * remainder) / (sketched.shape[0] * LANES) + 1e-06)
    scalars = jnp.where(lane == KRYLOV, norm, scalars)
    message = jnp.concatenate([remainder / norm, scalars], axis=0)
    for k in range(out_ref.shape[0]):
        out_ref[k] = message


def project(arrived, basis, count):
    return pl.pallas_call(
        project_kernel,
        out_shape=jax.ShapeDtypeStruct((count, arrived.shape[1] + 8, LANES), jnp.float32),
        in_specs=[VMEM] * 2,
        out_specs=VMEM,
        name="project",
        compiler_params=pltpu.CompilerParams(vmem_limit_bytes=4 * MIB),
    )(arrived, basis)


def finish_kernel(arrived_ref, image_ref, krylov_ref, next_ref, coefficients_ref, sketch_ref, norms_ref):
    rows = arrived_ref.shape[1] - 8
    for k in range(rows):
        sketch_ref[:, k * LANES : (k + 1) * LANES] = arrived_ref[:, k, :]
    scalars = arrived_ref[:, rows, :]
    reduced = image_ref[...]
    for j in range(KRYLOV):
        reduced = reduced - scalars[:, j : j + 1] * krylov_ref[j]
    next_ref[...] = reduced / scalars[:, KRYLOV : KRYLOV + 1]
    across = jnp.transpose(scalars)
    coefficients_ref[...] = across[0:KRYLOV, :]
    norms_ref[...] = across[KRYLOV : KRYLOV + 1, :]


def finish(arrived, image, krylov):
    rows = arrived.shape[1] - 8
    return pl.pallas_call(
        finish_kernel,
        out_shape=(
            jax.ShapeDtypeStruct((SYSTEMS, LANES), jnp.float32),
            jax.ShapeDtypeStruct((KRYLOV, SYSTEMS), jnp.float32),
            jax.ShapeDtypeStruct((SYSTEMS, rows * LANES), jnp.float32),
            jax.ShapeDtypeStruct((1, SYSTEMS), jnp.float32),
        ),
        in_specs=[VMEM] * 3,
        out_specs=(VMEM,) * 4,
        name="finish",
        compiler_params=pltpu.CompilerParams(vmem_limit_bytes=8 * MIB),
    )(arrived, image, krylov)


def shards(points, labels, shape_scale, krylov_basis, sketch, sketched_basis):
    everything = lax.axis_size(ALL) * points.shape[1]
    system = lax.axis_index(OWNERS)
    basis = lax.dynamic_slice_in_dim(sketched_basis, system, 1, axis=1)
    basis = basis.reshape(KRYLOV, -1, LANES)
    sources, targets = messages(points, labels, shape_scale, krylov_basis, lax.axis_size(ROW))
    all_sources = exchange(sources, ROW)
    all_targets = gather_by_distance(targets, COLUMN)
    all_targets, basis = lax.optimization_barrier((all_targets, basis))
    partial_value = pair_product(all_sources, all_targets)
    image, local_sketch = image_and_sketch(
        exchange(partial_value, COLUMN), sketch, math.sqrt(everything)
    )
    over_owners = sum_for_each(exchange(local_sketch, OWNERS), lax.axis_size(LAYERS))
    message = project(exchange(over_owners, LAYERS), basis, lax.axis_size(OWNERS))
    next_vector, coefficients, sketch_next, norms = finish(
        exchange(message, OWNERS), image, krylov_basis
    )
    return (next_vector, coefficients, sketch_next, norms.reshape(-1))


def solution(mesh):
    torus = Mesh(mesh.devices.reshape((2,) * len(ALL)), ALL)
    in_specs = (P(None, ALL), P(ALL), P(ALL), P(None, None, ALL), P(None, ALL), P())
    out_specs = (P(None, ALL), P(), P(), P())
    return jax.shard_map(
        shards, mesh=torus, in_specs=in_specs, out_specs=out_specs, check_vma=False
    )
```

```python
import functools
import math

import jax
import jax.numpy as jnp
from jax import lax
from jax.experimental import pallas as pl
from jax.experimental.pallas import tpu as pltpu
from jax.sharding import Mesh
from jax.sharding import PartitionSpec as P

SYSTEMS = 32
KRYLOV = 8
FEATS = 32
LANES = 128
X1, X0, Z2, Z1, Z0, Y1, Y0, CORE = ALL = ("x1", "x0", "z2", "z1", "z0", "y1", "y0", "core")
COLUMN = (Z1, Z0, Z2)
ROW = (X1, X0, Y1, Y0)
OWNERS = (X1, X0, Y1, Y0, CORE)
LAYERS = (Z2, Z1, Z0)
VMEM = pl.BlockSpec(memory_space=pltpu.VMEM)
MIB = 2**20


def exchange(value, axis):
    return lax.all_to_all(value, axis, 0, 0, tiled=True)


def swap(value, axis):
    return lax.ppermute(value, axis, ((0, 1), (1, 0)))


def gather_by_distance(value, axes):
    value = jnp.concatenate([value, swap(value, axes[-1])], axis=0)
    value = jnp.concatenate([value, swap(value, axes[-2])], axis=0)
    for axis in reversed(axes[:-2]):
        value = jnp.concatenate([value, swap(value, axis)], axis=0)
    return value


def parts(value):
    first = value.astype(jnp.bfloat16).astype(jnp.float32)
    rest = value - first
    second = rest.astype(jnp.bfloat16).astype(jnp.float32)
    return [first, second, rest - second]


def wide(tiles):
    return jnp.concatenate(tiles, axis=1)


def message_kernel(points_ref, labels_ref, scale_ref, krylov_ref, sources_ref, targets_ref, vector, row, copied, sem):
    taken = [
        pltpu.make_async_copy(krylov_ref.at[krylov_ref.shape[0] - 1], vector, sem.at[0]),
        pltpu.make_async_copy(points_ref, row.at[0:3], sem.at[1]),
        pltpu.make_async_copy(scale_ref, row.at[3:4], sem.at[2]),
        pltpu.make_async_copy(labels_ref, copied, sem.at[3]),
    ]
    for copy in taken:
        copy.start()
    for copy in taken:
        copy.wait()
    for k in range(sources_ref.shape[0]):
        sources_ref[k, 0:SYSTEMS, :] = vector[...]
        sources_ref[k, SYSTEMS : SYSTEMS + 4, :] = row[...]
    targets_ref[0, 0:3, :] = row[0:3, :]
    targets_ref[0, 3:4, :] = copied[...].astype(jnp.float32)


def messages(points, labels, shape_scale, krylov, count):
    hbm = pl.BlockSpec(memory_space=pltpu.HBM)
    return pl.pallas_call(
        message_kernel,
        out_shape=(
            jax.ShapeDtypeStruct((count, SYSTEMS + 4, LANES), jnp.float32),
            jax.ShapeDtypeStruct((1, 4, LANES), jnp.float32),
        ),
        in_specs=[hbm] * 4,
        out_specs=(VMEM,) * 2,
        scratch_shapes=[
            pltpu.VMEM((SYSTEMS, LANES), jnp.float32),
            pltpu.VMEM((4, LANES), jnp.float32),
            pltpu.VMEM((1, LANES), jnp.int32),
            pltpu.SemaphoreType.DMA((4,)),
        ],
        name="messages",
    )(points, labels[None, :], shape_scale[None, :], krylov)


def stored(rows, count, out_ref):
    zero = jnp.zeros((count, LANES), jnp.float32)
    for k, value in enumerate(rows + [zero] * (FEATS - len(rows))):
        out_ref[:, k, :] = value


def pair_kernel(unroll, *refs):
    (*source_refs, target_ref, out_ref, source_feats, target_feats, weights) = refs
    before_ref = None
    if len(source_refs) > 1:
        (*source_refs, before_ref) = source_refs
    for number, source_ref in enumerate(source_refs):
        count = source_ref.shape[0]
        coords = [source_ref[:, SYSTEMS + a, :] - 0.5 for a in range(3)]
        scale = source_ref[:, SYSTEMS + 3, :]
        per_square = 1.0 / (scale * scale)
        rows = []
        for value in [c * per_square for c in coords] + [per_square]:
            a, b, c = parts(value)
            rows += [a, a, b, b, a, c]
        square = coords[0] * coords[0] + coords[1] * coords[1] + coords[2] * coords[2]
        rows += parts(square * per_square + 1.0)
        stored(rows, count, source_feats.at[number * count : (number + 1) * count])
        for step in range(count // 2):
            weight = wide([source_ref[2 * step + j, 0:SYSTEMS, :] for j in range(2)])
            scale = wide([source_ref[2 * step + j, SYSTEMS + 3 : SYSTEMS + 4, :] for j in range(2)])
            inner, outer = weight / scale, weight * scale
            terms = []
            for value in (inner, outer):
                first = value.astype(jnp.bfloat16)
                terms += [first, (value - first.astype(jnp.float32)).astype(jnp.bfloat16)]
            weights[number * (count // 2) + step] = jnp.concatenate(terms, axis=0)
    owners = target_ref.shape[0]
    coords = [target_ref[:, a, :] - 0.5 for a in range(3)]
    square = coords[0] * coords[0] + coords[1] * coords[1] + coords[2] * coords[2]
    rows = []
    for value in [-2.0 * c for c in coords] + [square]:
        a, b, c = parts(value)
        rows += [a, b, a, b, c, a]
    rows += [jnp.ones((owners, LANES), jnp.float32)] * 3
    stored(rows, owners, target_feats)
    place = lax.axis_index(COLUMN)
    over_rows = (((0,), (0,)), ((), ()))

    def feats_of(ref, step):
        return wide([ref[2 * step], ref[2 * step + 1]]).astype(jnp.bfloat16)

    def over_targets(start, carry):
        for index in [start * unroll + k for k in range(unroll)]:
            feats = feats_of(target_feats, index)
            inner = wide([target_ref[2 * index + j, 3:4, :] for j in range(2)]) > 0.5
            total = jnp.zeros((4 * SYSTEMS, 2 * LANES), jnp.float32)
            for step in range(weights.shape[0]):
                ratio = lax.dot_general(
                    feats_of(source_feats, step), feats, over_rows, preferred_element_type=jnp.float32
                )
                root = lax.rsqrt(ratio)
                kernel = root * jnp.where(inner, 2.0 + root * root, ratio)
                first = kernel.astype(jnp.bfloat16)
                second = (kernel - first.astype(jnp.float32)).astype(jnp.bfloat16)
                weight = weights[step]
                total = (
                    total
                    + jnp.dot(weight, first, preferred_element_type=jnp.float32)
                    + jnp.dot(weight, second, preferred_element_type=jnp.float32)
                )
            a, b, c, d = (total[k * SYSTEMS : (k + 1) * SYSTEMS] for k in range(4))
            result = jnp.where(inner, a + b, c + d)
            for j in range(2):
                owner = jnp.bitwise_xor(place, 2 * index + j)
                part = result[:, j * LANES : (j + 1) * LANES]
                out_ref[owner] = part if before_ref is None else part + before_ref[owner]
        return carry

    lax.fori_loop(0, owners // 2 // unroll, over_targets, 0)


def pair_product(sources, targets, unroll=2):
    blocks, owners = sources[0].shape[0], targets.shape[0]
    pairs = blocks * owners * LANES * LANES
    return pl.pallas_call(
        functools.partial(pair_kernel, unroll),
        out_shape=jax.ShapeDtypeStruct((owners, SYSTEMS, LANES), jnp.float32),
        in_specs=[VMEM] * (len(sources) + 1),
        out_specs=VMEM,
        scratch_shapes=[
            pltpu.VMEM((blocks, FEATS, LANES), jnp.float32),
            pltpu.VMEM((owners, FEATS, LANES), jnp.float32),
            pltpu.VMEM((blocks // 2, 4 * SYSTEMS, 2 * LANES), jnp.bfloat16),
        ],
        cost_estimate=pl.CostEstimate(flops=6 * SYSTEMS * pairs, bytes_accessed=2**20, transcendentals=pairs),
        name="pairs",
        compiler_params=pltpu.CompilerParams(vmem_limit_bytes=16 * MIB),
    )(*sources, targets)


def image_kernel(root, arrived_ref, sketch_ref, image_ref, local_ref):
    total = arrived_ref[0]
    for k in range(1, arrived_ref.shape[0]):
        total = total + arrived_ref[k]
    image = total / root
    image_ref[...] = image
    for k in range(sketch_ref.shape[0] // LANES):
        local_ref[:, k, :] = lax.dot_general(
            image,
            sketch_ref[k * LANES : (k + 1) * LANES, :],
            (((1,), (1,)), ((), ())),
            precision=lax.Precision.HIGHEST,
            preferred_element_type=jnp.float32,
        )


def image_and_sketch(arrived, sketch, root):
    rows = sketch.shape[0]
    return pl.pallas_call(
        functools.partial(image_kernel, root),
        out_shape=(
            jax.ShapeDtypeStruct((SYSTEMS, LANES), jnp.float32),
            jax.ShapeDtypeStruct((SYSTEMS, rows // LANES, LANES), jnp.float32),
        ),
        in_specs=[VMEM] * 2,
        out_specs=(VMEM,) * 2,
        name="image",
        compiler_params=pltpu.CompilerParams(vmem_limit_bytes=8 * MIB),
    )(arrived, sketch)


def sum_kernel(arrived_ref, out_ref):
    total = arrived_ref[0]
    for k in range(1, arrived_ref.shape[0]):
        total = total + arrived_ref[k]
    for k in range(out_ref.shape[0]):
        out_ref[k] = total


def sum_for_each(arrived, count):
    return pl.pallas_call(
        sum_kernel,
        out_shape=jax.ShapeDtypeStruct((count, *arrived.shape[1:]), jnp.float32),
        in_specs=[VMEM],
        out_specs=VMEM,
        name="addup",
        compiler_params=pltpu.CompilerParams(vmem_limit_bytes=4 * MIB),
    )(arrived)


def project_kernel(arrived_ref, basis_ref, out_ref):
    sketched = arrived_ref[0]
    for k in range(1, arrived_ref.shape[0]):
        sketched = sketched + arrived_ref[k]
    lane = lax.broadcasted_iota(jnp.int32, (8, LANES), 1)

    def whole(value):
        return jnp.sum(jnp.sum(value, axis=1, keepdims=True), axis=0, keepdims=True)

    scalars = jnp.zeros((8, LANES), jnp.float32)
    remainder = sketched
    for j in range(KRYLOV):
        coefficient = whole(basis_ref[j] * sketched)
        scalars = jnp.where(lane == j, coefficient, scalars)
        remainder = remainder - coefficient * basis_ref[j]
    norm = jnp.sqrt(whole(remainder * remainder) / (sketched.shape[0] * LANES) + 1e-06)
    scalars = jnp.where(lane == KRYLOV, norm, scalars)
    message = jnp.concatenate([remainder / norm, scalars], axis=0)
    for k in range(out_ref.shape[0]):
        out_ref[k] = message


def project(arrived, basis, count):
    return pl.pallas_call(
        project_kernel,
        out_shape=jax.ShapeDtypeStruct((count, arrived.shape[1] + 8, LANES), jnp.float32),
        in_specs=[VMEM] * 2,
        out_specs=VMEM,
        name="project",
        compiler_params=pltpu.CompilerParams(vmem_limit_bytes=4 * MIB),
    )(arrived, basis)


def finish_kernel(arrived_ref, image_ref, krylov_ref, next_ref, coefficients_ref, sketch_ref, norms_ref):
    rows = arrived_ref.shape[1] - 8
    for k in range(rows):
        sketch_ref[:, k * LANES : (k + 1) * LANES] = arrived_ref[:, k, :]
    scalars = arrived_ref[:, rows, :]
    reduced = image_ref[...]
    for j in range(KRYLOV):
        reduced = reduced - scalars[:, j : j + 1] * krylov_ref[j]
    next_ref[...] = reduced / scalars[:, KRYLOV : KRYLOV + 1]
    across = jnp.transpose(scalars)
    coefficients_ref[...] = across[0:KRYLOV, :]
    norms_ref[...] = across[KRYLOV : KRYLOV + 1, :]


def finish(arrived, image, krylov):
    rows = arrived.shape[1] - 8
    return pl.pallas_call(
        finish_kernel,
        out_shape=(
            jax.ShapeDtypeStruct((SYSTEMS, LANES), jnp.float32),
            jax.ShapeDtypeStruct((KRYLOV, SYSTEMS), jnp.float32),
            jax.ShapeDtypeStruct((SYSTEMS, rows * LANES), jnp.float32),
            jax.ShapeDtypeStruct((1, SYSTEMS), jnp.float32),
        ),
        in_specs=[VMEM] * 3,
        out_specs=(VMEM,) * 4,
        name="finish",
        compiler_params=pltpu.CompilerParams(vmem_limit_bytes=8 * MIB),
    )(arrived, image, krylov)


def step(points, labels, shape_scale, krylov_basis, sketch, sketched_basis):
    everything = lax.axis_size(ALL) * points.shape[1]
    system = lax.axis_index(OWNERS)
    basis = lax.dynamic_slice_in_dim(sketched_basis, system, 1, axis=1)
    basis = basis.reshape(KRYLOV, -1, LANES)
    sources, targets = messages(points, labels, shape_scale, krylov_basis, lax.axis_size(ROW))
    all_sources = exchange(sources, ROW)
    all_targets = gather_by_distance(targets, COLUMN)
    all_targets, all_sources, basis = lax.optimization_barrier((all_targets, all_sources, basis))
    other_sources = swap(all_sources, CORE)
    partial_value = pair_product((all_sources,), all_targets)
    partial_value = pair_product((other_sources, partial_value), all_targets)
    image, local_sketch = image_and_sketch(
        exchange(partial_value, COLUMN), sketch, math.sqrt(everything)
    )
    over_owners = sum_for_each(exchange(local_sketch, OWNERS), lax.axis_size(LAYERS))
    message = project(exchange(over_owners, LAYERS), basis, lax.axis_size(OWNERS))
    next_vector, coefficients, sketch_next, norms = finish(
        exchange(message, OWNERS), image, krylov_basis
    )
    return (next_vector, coefficients, sketch_next, norms.reshape(-1))


def solution(mesh):
    torus = Mesh(mesh.devices.reshape((2,) * len(ALL)), ALL)
    in_specs = (P(None, ALL), P(ALL), P(ALL), P(None, None, ALL), P(None, ALL), P())
    out_specs = (P(None, ALL), P(), P(), P())
    return jax.shard_map(step, mesh=torus, in_specs=in_specs, out_specs=out_specs, check_vma=False)
```

```python
import functools
import math

import jax
import jax.numpy as jnp
from jax import lax
from jax.experimental import pallas as pl
from jax.experimental.pallas import tpu as pltpu
from jax.sharding import Mesh
from jax.sharding import PartitionSpec as P

SYSTEMS = 32
KRYLOV = 8
FEATS = 32
LANES = 128
X1, X0, Z2, Z1, Z0, Y1, Y0, CORE = ALL = ("x1", "x0", "z2", "z1", "z0", "y1", "y0", "core")
COLUMN = (Z2, Z0, Z1)
ROW = (X1, X0, Y1, Y0)
OWNERS = (X1, X0, Y1, Y0, CORE)
LAYERS = (Z2, Z1, Z0)
VMEM = pl.BlockSpec(memory_space=pltpu.VMEM)
MIB = 2**20


def exchange(value, axis):
    return lax.all_to_all(value, axis, 0, 0, tiled=True)


def swap(value, axis):
    return lax.ppermute(value, axis, ((0, 1), (1, 0)))


def with_other(value, axis):
    return jnp.concatenate([value, swap(value, axis)], axis=0)


def parts(value):
    first = value.astype(jnp.bfloat16).astype(jnp.float32)
    rest = value - first
    second = rest.astype(jnp.bfloat16).astype(jnp.float32)
    return [first, second, rest - second]


def wide(tiles):
    return jnp.concatenate(tiles, axis=1)


def message_kernel(points_ref, labels_ref, scale_ref, krylov_ref, sources_ref, targets_ref, vector, row, copied, sem):
    taken = [
        pltpu.make_async_copy(krylov_ref.at[krylov_ref.shape[0] - 1], vector, sem.at[0]),
        pltpu.make_async_copy(points_ref, row.at[0:3], sem.at[1]),
        pltpu.make_async_copy(scale_ref, row.at[3:4], sem.at[2]),
        pltpu.make_async_copy(labels_ref, copied, sem.at[3]),
    ]
    for copy in taken:
        copy.start()
    for copy in taken:
        copy.wait()
    for k in range(sources_ref.shape[0]):
        sources_ref[k, 0:SYSTEMS, :] = vector[...]
        sources_ref[k, SYSTEMS : SYSTEMS + 4, :] = row[...]
    targets_ref[0, 0:3, :] = row[0:3, :]
    targets_ref[0, 3:4, :] = copied[...].astype(jnp.float32)


def messages(points, labels, shape_scale, krylov, count):
    hbm = pl.BlockSpec(memory_space=pltpu.HBM)
    return pl.pallas_call(
        message_kernel,
        out_shape=(
            jax.ShapeDtypeStruct((count, SYSTEMS + 4, LANES), jnp.float32),
            jax.ShapeDtypeStruct((1, 4, LANES), jnp.float32),
        ),
        in_specs=[hbm] * 4,
        out_specs=(VMEM,) * 2,
        scratch_shapes=[
            pltpu.VMEM((SYSTEMS, LANES), jnp.float32),
            pltpu.VMEM((4, LANES), jnp.float32),
            pltpu.VMEM((1, LANES), jnp.int32),
            pltpu.SemaphoreType.DMA((4,)),
        ],
        name="messages",
    )(points, labels[None, :], shape_scale[None, :], krylov)


def stored(rows, out_ref):
    zero = jnp.zeros(rows[0].shape, jnp.float32)
    for k, value in enumerate(rows + [zero] * (FEATS - len(rows))):
        out_ref[:, k, :] = value


def pair_of(ref, step):
    return wide([ref[2 * step], ref[2 * step + 1]])


def describe_sources(source_ref, feats_ref, weights_ref):
    coords = [source_ref[:, SYSTEMS + a, :] - 0.5 for a in range(3)]
    scale = source_ref[:, SYSTEMS + 3, :]
    per_square = 1.0 / (scale * scale)
    rows = []
    for value in [c * per_square for c in coords] + [per_square]:
        a, b, c = parts(value)
        rows += [a, a, b, b, a, c]
    square = coords[0] * coords[0] + coords[1] * coords[1] + coords[2] * coords[2]
    stored(rows + parts(square * per_square + 1.0), feats_ref)
    for step in range(weights_ref.shape[0]):
        weight = wide([source_ref[2 * step + j, 0:SYSTEMS, :] for j in range(2)])
        scale = wide([source_ref[2 * step + j, SYSTEMS + 3 : SYSTEMS + 4, :] for j in range(2)])
        terms = []
        for value in (weight / scale, weight * scale):
            first = value.astype(jnp.bfloat16)
            terms += [first, (value - first.astype(jnp.float32)).astype(jnp.bfloat16)]
        weights_ref[step] = jnp.concatenate(terms, axis=0)


def describe_targets(target_ref, feats_ref):
    coords = [target_ref[:, a, :] - 0.5 for a in range(3)]
    square = coords[0] * coords[0] + coords[1] * coords[1] + coords[2] * coords[2]
    rows = []
    for value in [-2.0 * c for c in coords] + [square]:
        a, b, c = parts(value)
        rows += [a, b, a, b, c, a]
    stored(rows + [jnp.ones(square.shape, jnp.float32)] * 3, feats_ref)


def products(sources, target_ref, target_feats, index):
    feats = pair_of(target_feats, index).astype(jnp.bfloat16)
    inner = wide([target_ref[2 * index + j, 3:4, :] for j in range(2)]) > 0.5
    total = jnp.zeros((4 * SYSTEMS, 2 * LANES), jnp.float32)
    for source_feats, weights in sources:
        for step in range(weights.shape[0]):
            ratio = lax.dot_general(
                pair_of(source_feats, step).astype(jnp.bfloat16),
                feats,
                (((0,), (0,)), ((), ())),
                preferred_element_type=jnp.float32,
            )
            root = lax.rsqrt(ratio)
            kernel = root * jnp.where(inner, 2.0 + root * root, ratio)
            first = kernel.astype(jnp.bfloat16)
            second = (kernel - first.astype(jnp.float32)).astype(jnp.bfloat16)
            weight = weights[step]
            total = (
                total
                + jnp.dot(weight, first, preferred_element_type=jnp.float32)
                + jnp.dot(weight, second, preferred_element_type=jnp.float32)
            )
    a, b, c, d = (total[k * SYSTEMS : (k + 1) * SYSTEMS] for k in range(4))
    result = jnp.where(inner, a + b, c + d)
    return result[:, :LANES], result[:, LANES:]


def near_kernel(*refs):
    (source_ref, target_ref, *before, out_ref, source_feats, weights, target_feats) = refs
    describe_sources(source_ref, source_feats, weights)
    describe_targets(target_ref, target_feats)
    for index in range(target_ref.shape[0] // 2):
        for j, part in enumerate(products([(source_feats, weights)], target_ref, target_feats, index)):
            out_ref[2 * index + j] = part + before[0][2 * index + j] if before else part


def far_kernel(first_feats, first_weights, second_feats, second_weights, target_ref, near_ref, out_ref, target_feats):
    describe_targets(target_ref, target_feats)
    place = lax.axis_index(COLUMN)
    near = near_ref.shape[0]
    for k in range(near):
        out_ref[jnp.bitwise_xor(place, k)] = near_ref[k]
    sources = [(first_feats, first_weights), (second_feats, second_weights)]
    for index in range(target_ref.shape[0] // 2):
        for j, part in enumerate(products(sources, target_ref, target_feats, index)):
            out_ref[jnp.bitwise_xor(place, near + 2 * index + j)] = part


def cost(sources, targets):
    pairs = sources * targets * LANES * LANES
    return pl.CostEstimate(flops=12 * SYSTEMS * pairs, bytes_accessed=2**20, transcendentals=pairs)


def near_product(sources, targets, *before):
    blocks, owners = sources.shape[0], targets.shape[0]
    return pl.pallas_call(
        near_kernel,
        out_shape=(
            jax.ShapeDtypeStruct((owners, SYSTEMS, LANES), jnp.float32),
            jax.ShapeDtypeStruct((blocks, FEATS, LANES), jnp.float32),
            jax.ShapeDtypeStruct((blocks // 2, 4 * SYSTEMS, 2 * LANES), jnp.bfloat16),
        ),
        in_specs=[VMEM] * (2 + len(before)),
        out_specs=(VMEM,) * 3,
        scratch_shapes=[pltpu.VMEM((owners, FEATS, LANES), jnp.float32)],
        cost_estimate=cost(blocks, owners),
        name="near",
        compiler_params=pltpu.CompilerParams(vmem_limit_bytes=16 * MIB),
    )(sources, targets, *before)


def far_product(described, targets, near):
    blocks, owners = sum(feats.shape[0] for feats in described[::2]), targets.shape[0]
    return pl.pallas_call(
        far_kernel,
        out_shape=jax.ShapeDtypeStruct((owners + near.shape[0], SYSTEMS, LANES), jnp.float32),
        in_specs=[VMEM] * (len(described) + 2),
        out_specs=VMEM,
        scratch_shapes=[pltpu.VMEM((owners, FEATS, LANES), jnp.float32)],
        cost_estimate=cost(blocks, owners),
        name="far",
        compiler_params=pltpu.CompilerParams(vmem_limit_bytes=16 * MIB),
    )(*described, targets, near)


def image_kernel(root, arrived_ref, sketch_ref, image_ref, local_ref):
    total = arrived_ref[0]
    for k in range(1, arrived_ref.shape[0]):
        total = total + arrived_ref[k]
    image = total / root
    image_ref[...] = image
    first = image.astype(jnp.bfloat16)
    second = (image - first.astype(jnp.float32)).astype(jnp.bfloat16)
    both = jnp.concatenate([first, second], axis=0)
    over_lanes = (((1,), (1,)), ((), ()))
    for k in range(sketch_ref.shape[0] // (2 * LANES)):
        rows = sketch_ref[2 * k * LANES : 2 * (k + 1) * LANES, :]
        high = rows.astype(jnp.bfloat16)
        low = (rows - high.astype(jnp.float32)).astype(jnp.bfloat16)
        total = lax.dot_general(both, high, over_lanes, preferred_element_type=jnp.float32)
        total = total + lax.dot_general(both, low, over_lanes, preferred_element_type=jnp.float32)
        total = total[:SYSTEMS] + total[SYSTEMS:]
        for j in range(2):
            local_ref[:, 2 * k + j, :] = total[:, j * LANES : (j + 1) * LANES]


def image_and_sketch(arrived, sketch, root):
    rows = sketch.shape[0]
    return pl.pallas_call(
        functools.partial(image_kernel, root),
        out_shape=(
            jax.ShapeDtypeStruct((SYSTEMS, LANES), jnp.float32),
            jax.ShapeDtypeStruct((SYSTEMS, rows // LANES, LANES), jnp.float32),
        ),
        in_specs=[VMEM] * 2,
        out_specs=(VMEM,) * 2,
        name="image",
        compiler_params=pltpu.CompilerParams(vmem_limit_bytes=8 * MIB),
    )(arrived, sketch)


def sum_kernel(arrived_ref, out_ref):
    total = arrived_ref[0]
    for k in range(1, arrived_ref.shape[0]):
        total = total + arrived_ref[k]
    for k in range(out_ref.shape[0]):
        out_ref[k] = total


def sum_for_each(arrived, count):
    return pl.pallas_call(
        sum_kernel,
        out_shape=jax.ShapeDtypeStruct((count, *arrived.shape[1:]), jnp.float32),
        in_specs=[VMEM],
        out_specs=VMEM,
        name="addup",
        compiler_params=pltpu.CompilerParams(vmem_limit_bytes=4 * MIB),
    )(arrived)


def project_kernel(arrived_ref, basis_ref, out_ref):
    sketched = arrived_ref[0]
    for k in range(1, arrived_ref.shape[0]):
        sketched = sketched + arrived_ref[k]
    lane = lax.broadcasted_iota(jnp.int32, (8, LANES), 1)

    def whole(value):
        return jnp.sum(jnp.sum(value, axis=1, keepdims=True), axis=0, keepdims=True)

    scalars = jnp.zeros((8, LANES), jnp.float32)
    remainder = sketched
    for j in range(KRYLOV):
        coefficient = whole(basis_ref[j] * sketched)
        scalars = jnp.where(lane == j, coefficient, scalars)
        remainder = remainder - coefficient * basis_ref[j]
    norm = jnp.sqrt(whole(remainder * remainder) / (sketched.shape[0] * LANES) + 1e-06)
    scalars = jnp.where(lane == KRYLOV, norm, scalars)
    message = jnp.concatenate([remainder / norm, scalars[0:1, :]], axis=0)
    for k in range(out_ref.shape[0]):
        for j in range(message.shape[0]):
            out_ref[k, :, j * LANES : (j + 1) * LANES] = message[j : j + 1, :]


def project(arrived, basis, count):
    return pl.pallas_call(
        project_kernel,
        out_shape=jax.ShapeDtypeStruct((count, 1, (arrived.shape[1] + 1) * LANES), jnp.float32),
        in_specs=[VMEM] * 2,
        out_specs=VMEM,
        name="project",
        compiler_params=pltpu.CompilerParams(vmem_limit_bytes=4 * MIB),
    )(arrived, basis)


def finish_kernel(arrived_ref, image_ref, krylov_ref, next_ref, coefficients_ref, sketch_ref, norms_ref):
    width = sketch_ref.shape[1]
    sketch_ref[...] = arrived_ref[:, 0, :width]
    scalars = arrived_ref[:, 0, width:]
    reduced = image_ref[...]
    for j in range(KRYLOV):
        reduced = reduced - scalars[:, j : j + 1] * krylov_ref[j]
    next_ref[...] = reduced / scalars[:, KRYLOV : KRYLOV + 1]
    across = jnp.transpose(scalars)
    coefficients_ref[...] = across[0:KRYLOV, :]
    norms_ref[...] = across[KRYLOV : KRYLOV + 1, :]


def finish(arrived, image, krylov):
    width = arrived.shape[2] - LANES
    return pl.pallas_call(
        finish_kernel,
        out_shape=(
            jax.ShapeDtypeStruct((SYSTEMS, LANES), jnp.float32),
            jax.ShapeDtypeStruct((KRYLOV, SYSTEMS), jnp.float32),
            jax.ShapeDtypeStruct((SYSTEMS, width), jnp.float32),
            jax.ShapeDtypeStruct((1, SYSTEMS), jnp.float32),
        ),
        in_specs=[VMEM] * 3,
        out_specs=(VMEM,) * 4,
        name="finish",
        compiler_params=pltpu.CompilerParams(vmem_limit_bytes=8 * MIB),
    )(arrived, image, krylov)


def step(points, labels, shape_scale, krylov_basis, sketch, sketched_basis):
    everything = lax.axis_size(ALL) * points.shape[1]
    system = lax.axis_index(OWNERS)
    basis = lax.dynamic_slice_in_dim(sketched_basis, system, 1, axis=1)
    basis = basis.reshape(KRYLOV, -1, LANES)
    sources, targets = messages(points, labels, shape_scale, krylov_basis, lax.axis_size(ROW))
    all_sources = exchange(sources, ROW)
    near = with_other(targets, COLUMN[2])
    near = with_other(near, COLUMN[1])
    far = swap(near, COLUMN[0])
    near, all_sources, basis = lax.optimization_barrier((near, all_sources, basis))
    other_sources = swap(all_sources, CORE)
    partial_value, *first = near_product(all_sources, near)
    partial_value, *second = near_product(other_sources, near, partial_value)
    partial_value = far_product((*first, *second), far, partial_value)
    image, local_sketch = image_and_sketch(
        exchange(partial_value, COLUMN), sketch, math.sqrt(everything)
    )
    over_owners = sum_for_each(exchange(local_sketch, OWNERS), lax.axis_size(LAYERS))
    message = project(exchange(over_owners, LAYERS), basis, lax.axis_size(OWNERS))
    next_vector, coefficients, sketch_next, norms = finish(
        exchange(message, OWNERS), image, krylov_basis
    )
    return (next_vector, coefficients, sketch_next, norms.reshape(-1))


def solution(mesh):
    torus = Mesh(mesh.devices.reshape((2,) * len(ALL)), ALL)
    in_specs = (P(None, ALL), P(ALL), P(ALL), P(None, None, ALL), P(None, ALL), P())
    out_specs = (P(None, ALL), P(), P(), P())
    return jax.shard_map(step, mesh=torus, in_specs=in_specs, out_specs=out_specs, check_vma=False)
```

```python
import functools
import math

import jax
import jax.numpy as jnp
from jax import lax
from jax.experimental import pallas as pl
from jax.experimental.pallas import tpu as pltpu
from jax.sharding import Mesh
from jax.sharding import PartitionSpec as P

SYSTEMS = 32
KRYLOV = 8
FEATS = 32
LANES = 128
X1, X0, Z2, Z1, Z0, Y1, Y0, CORE = ALL = ("x1", "x0", "z2", "z1", "z0", "y1", "y0", "core")
COLUMN = (Z2, Z0, Z1)
ROW = (X1, X0, Y1, Y0)
OWNERS = (X1, X0, Y0, CORE)
LAYERS = (Y1, Z2, Z1, Z0)
VMEM = pl.BlockSpec(memory_space=pltpu.VMEM)
MIB = 2**20


def exchange(value, axis):
    return lax.all_to_all(value, axis, 0, 0, tiled=True)


def swap(value, axis):
    return lax.ppermute(value, axis, ((0, 1), (1, 0)))


def with_other(value, axis):
    return jnp.concatenate([value, swap(value, axis)], axis=0)


def parts(value):
    first = value.astype(jnp.bfloat16).astype(jnp.float32)
    rest = value - first
    second = rest.astype(jnp.bfloat16).astype(jnp.float32)
    return [first, second, rest - second]


def wide(tiles):
    return jnp.concatenate(tiles, axis=1)


def message_kernel(points_ref, labels_ref, scale_ref, krylov_ref, sources_ref, targets_ref, vector, row, copied, sem):
    taken = [
        pltpu.make_async_copy(krylov_ref.at[krylov_ref.shape[0] - 1], vector, sem.at[0]),
        pltpu.make_async_copy(points_ref, row.at[0:3], sem.at[1]),
        pltpu.make_async_copy(scale_ref, row.at[3:4], sem.at[2]),
        pltpu.make_async_copy(labels_ref, copied, sem.at[3]),
    ]
    for copy in taken:
        copy.start()
    for copy in taken:
        copy.wait()
    for k in range(sources_ref.shape[0]):
        sources_ref[k, 0:SYSTEMS, :] = vector[...]
        sources_ref[k, SYSTEMS : SYSTEMS + 4, :] = row[...]
    targets_ref[0, 0:3, :] = row[0:3, :]
    targets_ref[0, 3:4, :] = copied[...].astype(jnp.float32)


def messages(points, labels, shape_scale, krylov, count):
    hbm = pl.BlockSpec(memory_space=pltpu.HBM)
    return pl.pallas_call(
        message_kernel,
        out_shape=(
            jax.ShapeDtypeStruct((count, SYSTEMS + 4, LANES), jnp.float32),
            jax.ShapeDtypeStruct((1, 4, LANES), jnp.float32),
        ),
        in_specs=[hbm] * 4,
        out_specs=(VMEM,) * 2,
        scratch_shapes=[
            pltpu.VMEM((SYSTEMS, LANES), jnp.float32),
            pltpu.VMEM((4, LANES), jnp.float32),
            pltpu.VMEM((1, LANES), jnp.int32),
            pltpu.SemaphoreType.DMA((4,)),
        ],
        name="messages",
    )(points, labels[None, :], shape_scale[None, :], krylov)


def stored(rows, out_ref):
    zero = jnp.zeros(rows[0].shape, jnp.float32)
    for k, value in enumerate(rows + [zero] * (FEATS - len(rows))):
        out_ref[:, k, :] = value


def pair_of(ref, step):
    return wide([ref[2 * step], ref[2 * step + 1]])


def describe_sources(source_ref, feats_ref, weights_ref):
    coords = [source_ref[:, SYSTEMS + a, :] - 0.5 for a in range(3)]
    scale = source_ref[:, SYSTEMS + 3, :]
    per_square = 1.0 / (scale * scale)
    rows = []
    for value in [c * per_square for c in coords] + [per_square]:
        a, b, c = parts(value)
        rows += [a, a, b, b, a, c]
    square = coords[0] * coords[0] + coords[1] * coords[1] + coords[2] * coords[2]
    stored(rows + parts(square * per_square + 1.0), feats_ref)
    for step in range(weights_ref.shape[0]):
        weight = wide([source_ref[2 * step + j, 0:SYSTEMS, :] for j in range(2)])
        scale = wide([source_ref[2 * step + j, SYSTEMS + 3 : SYSTEMS + 4, :] for j in range(2)])
        terms = []
        for value in (weight / scale, weight * scale):
            first = value.astype(jnp.bfloat16)
            terms += [first, (value - first.astype(jnp.float32)).astype(jnp.bfloat16)]
        weights_ref[step] = jnp.concatenate(terms, axis=0)


def describe_targets(target_ref, feats_ref):
    coords = [target_ref[:, a, :] - 0.5 for a in range(3)]
    square = coords[0] * coords[0] + coords[1] * coords[1] + coords[2] * coords[2]
    rows = []
    for value in [-2.0 * c for c in coords] + [square]:
        a, b, c = parts(value)
        rows += [a, b, a, b, c, a]
    stored(rows + [jnp.ones(square.shape, jnp.float32)] * 3, feats_ref)


def products(sources, target_ref, target_feats, index):
    feats = pair_of(target_feats, index).astype(jnp.bfloat16)
    inner = wide([target_ref[2 * index + j, 3:4, :] for j in range(2)]) > 0.5
    total = jnp.zeros((4 * SYSTEMS, 2 * LANES), jnp.float32)
    for source_feats, weights in sources:
        for step in range(weights.shape[0]):
            ratio = lax.dot_general(
                pair_of(source_feats, step).astype(jnp.bfloat16),
                feats,
                (((0,), (0,)), ((), ())),
                preferred_element_type=jnp.float32,
            )
            root = lax.rsqrt(ratio)
            kernel = root * jnp.where(inner, 2.0 + root * root, ratio)
            first = kernel.astype(jnp.bfloat16)
            second = (kernel - first.astype(jnp.float32)).astype(jnp.bfloat16)
            weight = weights[step]
            total = (
                total
                + jnp.dot(weight, first, preferred_element_type=jnp.float32)
                + jnp.dot(weight, second, preferred_element_type=jnp.float32)
            )
    a, b, c, d = (total[k * SYSTEMS : (k + 1) * SYSTEMS] for k in range(4))
    result = jnp.where(inner, a + b, c + d)
    return result[:, :LANES], result[:, LANES:]


def near_kernel(*refs):
    (source_ref, target_ref, *before, out_ref, source_feats, weights, target_feats) = refs
    describe_sources(source_ref, source_feats, weights)
    describe_targets(target_ref, target_feats)
    for index in range(target_ref.shape[0] // 2):
        for j, part in enumerate(products([(source_feats, weights)], target_ref, target_feats, index)):
            out_ref[2 * index + j] = part + before[0][2 * index + j] if before else part


def far_kernel(first_feats, first_weights, second_feats, second_weights, target_ref, near_ref, out_ref, target_feats):
    describe_targets(target_ref, target_feats)
    place = lax.axis_index(COLUMN)
    near = near_ref.shape[0]
    for k in range(near):
        out_ref[jnp.bitwise_xor(place, k)] = near_ref[k]
    sources = [(first_feats, first_weights), (second_feats, second_weights)]
    for index in range(target_ref.shape[0] // 2):
        for j, part in enumerate(products(sources, target_ref, target_feats, index)):
            out_ref[jnp.bitwise_xor(place, near + 2 * index + j)] = part


def cost(sources, targets):
    pairs = sources * targets * LANES * LANES
    return pl.CostEstimate(flops=12 * SYSTEMS * pairs, bytes_accessed=2**20, transcendentals=pairs)


def near_product(sources, targets, *before):
    blocks, owners = sources.shape[0], targets.shape[0]
    return pl.pallas_call(
        near_kernel,
        out_shape=(
            jax.ShapeDtypeStruct((owners, SYSTEMS, LANES), jnp.float32),
            jax.ShapeDtypeStruct((blocks, FEATS, LANES), jnp.float32),
            jax.ShapeDtypeStruct((blocks // 2, 4 * SYSTEMS, 2 * LANES), jnp.bfloat16),
        ),
        in_specs=[VMEM] * (2 + len(before)),
        out_specs=(VMEM,) * 3,
        scratch_shapes=[pltpu.VMEM((owners, FEATS, LANES), jnp.float32)],
        cost_estimate=cost(blocks, owners),
        name="near",
        compiler_params=pltpu.CompilerParams(vmem_limit_bytes=16 * MIB),
    )(sources, targets, *before)


def far_product(described, targets, near):
    blocks, owners = sum(feats.shape[0] for feats in described[::2]), targets.shape[0]
    return pl.pallas_call(
        far_kernel,
        out_shape=jax.ShapeDtypeStruct((owners + near.shape[0], SYSTEMS, LANES), jnp.float32),
        in_specs=[VMEM] * (len(described) + 2),
        out_specs=VMEM,
        scratch_shapes=[pltpu.VMEM((owners, FEATS, LANES), jnp.float32)],
        cost_estimate=cost(blocks, owners),
        name="far",
        compiler_params=pltpu.CompilerParams(vmem_limit_bytes=16 * MIB),
    )(*described, targets, near)


def image_kernel(root, arrived_ref, sketch_ref, image_ref, local_ref):
    total = arrived_ref[0]
    for k in range(1, arrived_ref.shape[0]):
        total = total + arrived_ref[k]
    image = total / root
    image_ref[...] = image
    first = image.astype(jnp.bfloat16)
    second = (image - first.astype(jnp.float32)).astype(jnp.bfloat16)
    both = jnp.concatenate([first, second], axis=0)
    over_lanes = (((1,), (1,)), ((), ()))
    for k in range(sketch_ref.shape[0] // (2 * LANES)):
        rows = sketch_ref[2 * k * LANES : 2 * (k + 1) * LANES, :]
        high = rows.astype(jnp.bfloat16)
        low = (rows - high.astype(jnp.float32)).astype(jnp.bfloat16)
        total = lax.dot_general(both, high, over_lanes, preferred_element_type=jnp.float32)
        total = total + lax.dot_general(both, low, over_lanes, preferred_element_type=jnp.float32)
        total = total[:SYSTEMS] + total[SYSTEMS:]
        for j in range(2):
            local_ref[:, 2 * k + j, :] = total[:, j * LANES : (j + 1) * LANES]


def image_and_sketch(arrived, sketch, root):
    rows = sketch.shape[0]
    return pl.pallas_call(
        functools.partial(image_kernel, root),
        out_shape=(
            jax.ShapeDtypeStruct((SYSTEMS, LANES), jnp.float32),
            jax.ShapeDtypeStruct((SYSTEMS, rows // LANES, LANES), jnp.float32),
        ),
        in_specs=[VMEM] * 2,
        out_specs=(VMEM,) * 2,
        name="image",
        compiler_params=pltpu.CompilerParams(vmem_limit_bytes=8 * MIB),
    )(arrived, sketch)


def sum_kernel(arrived_ref, out_ref):
    total = arrived_ref[0]
    for k in range(1, arrived_ref.shape[0]):
        total = total + arrived_ref[k]
    for k in range(out_ref.shape[0]):
        out_ref[k] = total


def sum_for_each(arrived, count):
    return pl.pallas_call(
        sum_kernel,
        out_shape=jax.ShapeDtypeStruct((count, *arrived.shape[1:]), jnp.float32),
        in_specs=[VMEM],
        out_specs=VMEM,
        name="addup",
        compiler_params=pltpu.CompilerParams(vmem_limit_bytes=4 * MIB),
    )(arrived)


def project_kernel(share, arrived_ref, basis_ref, out_ref):
    total = arrived_ref[0]
    for k in range(1, arrived_ref.shape[0]):
        total = total + arrived_ref[k]
    rows = total.shape[0] // share
    lane = lax.broadcasted_iota(jnp.int32, (1, LANES), 1)

    def whole(value):
        return jnp.sum(jnp.sum(value, axis=1, keepdims=True), axis=0, keepdims=True)

    lines, last = [], []
    for part in range(share):
        sketched = total[part * rows : (part + 1) * rows]
        basis = [basis_ref[j, part * rows : (part + 1) * rows, :] for j in range(KRYLOV)]
        scalars = jnp.zeros((1, LANES), jnp.float32)
        remainder = sketched
        for j in range(KRYLOV):
            coefficient = whole(basis[j] * sketched)
            scalars = jnp.where(lane == j, coefficient, scalars)
            remainder = remainder - coefficient * basis[j]
        norm = jnp.sqrt(whole(remainder * remainder) / (rows * LANES) + 1e-06)
        lines.append(remainder / norm)
        last.append(jnp.where(lane == KRYLOV, norm, scalars))
    message = jnp.concatenate(lines + last, axis=0)
    for k in range(out_ref.shape[0]):
        for j in range(message.shape[0]):
            out_ref[k, :, j * LANES : (j + 1) * LANES] = message[j : j + 1, :]


def project(arrived, basis, count):
    share = SYSTEMS // count
    return pl.pallas_call(
        functools.partial(project_kernel, share),
        out_shape=jax.ShapeDtypeStruct((count, 1, (arrived.shape[1] + share) * LANES), jnp.float32),
        in_specs=[VMEM] * 2,
        out_specs=VMEM,
        name="project",
        compiler_params=pltpu.CompilerParams(vmem_limit_bytes=4 * MIB),
    )(arrived, basis)


def finish_kernel(arrived_ref, image_ref, krylov_ref, next_ref, coefficients_ref, sketch_ref, norms_ref, lines):
    width, count = sketch_ref.shape[1], arrived_ref.shape[0]
    share = SYSTEMS // count
    for part in range(share):
        place = pl.ds(part, count, stride=share)
        for k in range(width // LANES):
            at = part * width + k * LANES
            lines[k, place, :] = arrived_ref[:, 0, at : at + LANES]
        at = share * width + part * LANES
        lines[width // LANES, place, :] = arrived_ref[:, 0, at : at + LANES]
    for k in range(width // LANES):
        sketch_ref[:, k * LANES : (k + 1) * LANES] = lines[k]
    scalars = lines[width // LANES]
    reduced = image_ref[...]
    for j in range(KRYLOV):
        reduced = reduced - scalars[:, j : j + 1] * krylov_ref[j]
    next_ref[...] = reduced / scalars[:, KRYLOV : KRYLOV + 1]
    across = jnp.transpose(scalars)
    coefficients_ref[...] = across[0:KRYLOV, :]
    norms_ref[...] = across[KRYLOV : KRYLOV + 1, :]


def finish(arrived, image, krylov):
    width = arrived.shape[2] * arrived.shape[0] // SYSTEMS - LANES
    return pl.pallas_call(
        finish_kernel,
        out_shape=(
            jax.ShapeDtypeStruct((SYSTEMS, LANES), jnp.float32),
            jax.ShapeDtypeStruct((KRYLOV, SYSTEMS), jnp.float32),
            jax.ShapeDtypeStruct((SYSTEMS, width), jnp.float32),
            jax.ShapeDtypeStruct((1, SYSTEMS), jnp.float32),
        ),
        in_specs=[VMEM] * 3,
        out_specs=(VMEM,) * 4,
        scratch_shapes=[pltpu.VMEM((width // LANES + 1, SYSTEMS, LANES), jnp.float32)],
        name="finish",
        compiler_params=pltpu.CompilerParams(vmem_limit_bytes=8 * MIB),
    )(arrived, image, krylov)


def step(points, labels, shape_scale, krylov_basis, sketch, sketched_basis):
    everything = lax.axis_size(ALL) * points.shape[1]
    system = lax.axis_index(OWNERS)
    share = SYSTEMS // lax.axis_size(OWNERS)
    basis = lax.dynamic_slice_in_dim(sketched_basis, system * share, share, axis=1)
    basis = basis.reshape(KRYLOV, -1, LANES)
    sources, targets = messages(points, labels, shape_scale, krylov_basis, lax.axis_size(ROW))
    all_sources = exchange(sources, ROW)
    near = with_other(targets, COLUMN[2])
    near = with_other(near, COLUMN[1])
    far = swap(near, COLUMN[0])
    near, all_sources, basis = lax.optimization_barrier((near, all_sources, basis))
    other_sources = swap(all_sources, CORE)
    partial_value, *first = near_product(all_sources, near)
    partial_value, *second = near_product(other_sources, near, partial_value)
    partial_value = far_product((*first, *second), far, partial_value)
    image, local_sketch = image_and_sketch(
        exchange(partial_value, COLUMN), sketch, math.sqrt(everything)
    )
    local_sketch = local_sketch.reshape(lax.axis_size(OWNERS), -1, LANES)
    over_owners = sum_for_each(exchange(local_sketch, OWNERS), lax.axis_size(LAYERS))
    message = project(exchange(over_owners, LAYERS), basis, lax.axis_size(OWNERS))
    next_vector, coefficients, sketch_next, norms = finish(
        exchange(message, OWNERS), image, krylov_basis
    )
    return (next_vector, coefficients, sketch_next, norms.reshape(-1))


def solution(mesh):
    torus = Mesh(mesh.devices.reshape((2,) * len(ALL)), ALL)
    in_specs = (P(None, ALL), P(ALL), P(ALL), P(None, None, ALL), P(None, ALL), P())
    out_specs = (P(None, ALL), P(), P(), P())
    return jax.shard_map(step, mesh=torus, in_specs=in_specs, out_specs=out_specs, check_vma=False)
```

```python
import functools
import math

import jax
import jax.numpy as jnp
from jax import lax
from jax.experimental import pallas as pl
from jax.experimental.pallas import tpu as pltpu
from jax.sharding import Mesh
from jax.sharding import PartitionSpec as P

SYSTEMS = 32
KRYLOV = 8
FEATS = 32
LANES = 128
X1, X0, Z2, Z1, Z0, Y1, Y0, CORE = ALL = ("x1", "x0", "z2", "z1", "z0", "y1", "y0", "core")
COLUMN = (Z2, Z1, Z0)
ROW = (X1, X0, Y1, Y0)
OWNERS = (X1, X0, Y0, CORE)
LAYERS = (Y1, Y0, Z2, Z1, Z0)
PAIRS = tuple(tuple(8 * y + z for y in pair for z in range(8)) for pair in ((0, 3), (1, 2)))
VMEM = pl.BlockSpec(memory_space=pltpu.VMEM)
MIB = 2**20


def exchange(value, axis):
    return lax.all_to_all(value, axis, 0, 0, tiled=True)


def exchange_layers(value):
    return lax.all_to_all(value, LAYERS, 0, 0, axis_index_groups=PAIRS, tiled=True)


def in_order(value):
    rows = value.shape[0]
    swapped = jnp.concatenate([value[k ^ 4 : (k ^ 4) + 4] for k in range(0, rows, 4)], axis=0)
    return jnp.where(lax.axis_index(Y1) == 1, swapped, value)


def swap(value, axis):
    return lax.ppermute(value, axis, ((0, 1), (1, 0)))


def with_other(value, axis):
    return jnp.concatenate([value, swap(value, axis)], axis=0)


def parts(value):
    first = value.astype(jnp.bfloat16).astype(jnp.float32)
    rest = value - first
    second = rest.astype(jnp.bfloat16).astype(jnp.float32)
    return [first, second, rest - second]


def wide(tiles):
    return jnp.concatenate(tiles, axis=1)


def message_kernel(points_ref, labels_ref, scale_ref, krylov_ref, sources_ref, targets_ref, vector, row, copied, sem):
    taken = [
        pltpu.make_async_copy(krylov_ref.at[krylov_ref.shape[0] - 1], vector, sem.at[0]),
        pltpu.make_async_copy(points_ref, row.at[0:3], sem.at[1]),
        pltpu.make_async_copy(scale_ref, row.at[3:4], sem.at[2]),
        pltpu.make_async_copy(labels_ref, copied, sem.at[3]),
    ]
    for copy in taken:
        copy.start()
    for copy in taken:
        copy.wait()
    for k in range(sources_ref.shape[0]):
        sources_ref[k, 0:SYSTEMS, :] = vector[...]
        sources_ref[k, SYSTEMS : SYSTEMS + 4, :] = row[...]
    targets_ref[0, 0:3, :] = row[0:3, :]
    targets_ref[0, 3:4, :] = copied[...].astype(jnp.float32)


def messages(points, labels, shape_scale, krylov, count):
    hbm = pl.BlockSpec(memory_space=pltpu.HBM)
    return pl.pallas_call(
        message_kernel,
        out_shape=(
            jax.ShapeDtypeStruct((count, SYSTEMS + 4, LANES), jnp.float32),
            jax.ShapeDtypeStruct((1, 4, LANES), jnp.float32),
        ),
        in_specs=[hbm] * 4,
        out_specs=(VMEM,) * 2,
        scratch_shapes=[
            pltpu.VMEM((SYSTEMS, LANES), jnp.float32),
            pltpu.VMEM((4, LANES), jnp.float32),
            pltpu.VMEM((1, LANES), jnp.int32),
            pltpu.SemaphoreType.DMA((4,)),
        ],
        name="messages",
    )(points, labels[None, :], shape_scale[None, :], krylov)


def stored(rows, out_ref):
    zero = jnp.zeros(rows[0].shape, jnp.float32)
    for k, value in enumerate(rows + [zero] * (FEATS - len(rows))):
        out_ref[:, k, :] = value


def pair_of(ref, step):
    return wide([ref[2 * step], ref[2 * step + 1]])


def describe_sources(source_ref, feats_ref, weights_ref):
    coords = [source_ref[:, SYSTEMS + a, :] - 0.5 for a in range(3)]
    scale = source_ref[:, SYSTEMS + 3, :]
    per_square = 1.0 / (scale * scale)
    rows = []
    for value in [c * per_square for c in coords] + [per_square]:
        a, b, c = parts(value)
        rows += [a, a, b, b, a, c]
    square = coords[0] * coords[0] + coords[1] * coords[1] + coords[2] * coords[2]
    stored(rows + parts(square * per_square + 1.0), feats_ref)
    for step in range(weights_ref.shape[0]):
        weight = wide([source_ref[2 * step + j, 0:SYSTEMS, :] for j in range(2)])
        scale = wide([source_ref[2 * step + j, SYSTEMS + 3 : SYSTEMS + 4, :] for j in range(2)])
        terms = []
        for value in (weight / scale, weight * scale):
            first = value.astype(jnp.bfloat16)
            terms += [first, (value - first.astype(jnp.float32)).astype(jnp.bfloat16)]
        weights_ref[step] = jnp.concatenate(terms, axis=0)


def describe_targets(target_ref, feats_ref):
    coords = [target_ref[:, a, :] - 0.5 for a in range(3)]
    square = coords[0] * coords[0] + coords[1] * coords[1] + coords[2] * coords[2]
    rows = []
    for value in [-2.0 * c for c in coords] + [square]:
        a, b, c = parts(value)
        rows += [a, b, a, b, c, a]
    stored(rows + [jnp.ones(square.shape, jnp.float32)] * 3, feats_ref)


def products(sources, target_ref, target_feats):
    indices = range(target_ref.shape[0] // 2)
    feats = [pair_of(target_feats, index).astype(jnp.bfloat16) for index in indices]
    inner = [wide([target_ref[2 * index + j, 3:4, :] for j in range(2)]) > 0.5 for index in indices]
    totals = [jnp.zeros((4 * SYSTEMS, 2 * LANES), jnp.float32) for index in indices]
    for source_feats, weights in sources:
        for step in range(weights.shape[0]):
            source = pair_of(source_feats, step).astype(jnp.bfloat16)
            weight = weights[step]
            for index in indices:
                ratio = lax.dot_general(
                    source, feats[index], (((0,), (0,)), ((), ())), preferred_element_type=jnp.float32
                )
                root = lax.rsqrt(ratio)
                kernel = root * jnp.where(inner[index], 2.0 + root * root, ratio)
                first = kernel.astype(jnp.bfloat16)
                second = (kernel - first.astype(jnp.float32)).astype(jnp.bfloat16)
                totals[index] = (
                    totals[index]
                    + jnp.dot(weight, first, preferred_element_type=jnp.float32)
                    + jnp.dot(weight, second, preferred_element_type=jnp.float32)
                )
    results = []
    for index in indices:
        a, b, c, d = (totals[index][k * SYSTEMS : (k + 1) * SYSTEMS] for k in range(4))
        result = jnp.where(inner[index], a + b, c + d)
        results += [result[:, :LANES], result[:, LANES:]]
    return results


def near_kernel(*refs):
    (source_ref, target_ref, *before, out_ref, source_feats, weights, target_feats) = refs
    describe_sources(source_ref, source_feats, weights)
    describe_targets(target_ref, target_feats)
    for k, part in enumerate(products([(source_feats, weights)], target_ref, target_feats)):
        out_ref[k] = part + before[0][k] if before else part


def far_kernel(first_feats, first_weights, second_feats, second_weights, target_ref, near_ref, out_ref, target_feats):
    describe_targets(target_ref, target_feats)
    place = lax.axis_index(COLUMN)
    near = near_ref.shape[0]
    for k in range(near):
        out_ref[jnp.bitwise_xor(place, k)] = near_ref[k]
    sources = [(first_feats, first_weights), (second_feats, second_weights)]
    for k, part in enumerate(products(sources, target_ref, target_feats)):
        out_ref[jnp.bitwise_xor(place, (near + 2) ^ k)] = part


def cost(sources, targets):
    pairs = sources * targets * LANES * LANES
    return pl.CostEstimate(flops=12 * SYSTEMS * pairs, bytes_accessed=2**20, transcendentals=pairs)


def near_product(sources, targets, *before):
    blocks, owners = sources.shape[0], targets.shape[0]
    return pl.pallas_call(
        near_kernel,
        out_shape=(
            jax.ShapeDtypeStruct((owners, SYSTEMS, LANES), jnp.float32),
            jax.ShapeDtypeStruct((blocks, FEATS, LANES), jnp.float32),
            jax.ShapeDtypeStruct((blocks // 2, 4 * SYSTEMS, 2 * LANES), jnp.bfloat16),
        ),
        in_specs=[VMEM] * (2 + len(before)),
        out_specs=(VMEM,) * 3,
        scratch_shapes=[pltpu.VMEM((owners, FEATS, LANES), jnp.float32)],
        cost_estimate=cost(blocks, owners),
        name="near",
        compiler_params=pltpu.CompilerParams(vmem_limit_bytes=16 * MIB),
    )(sources, targets, *before)


def far_product(described, targets, near):
    blocks, owners = sum(feats.shape[0] for feats in described[::2]), targets.shape[0]
    return pl.pallas_call(
        far_kernel,
        out_shape=jax.ShapeDtypeStruct((owners + near.shape[0], SYSTEMS, LANES), jnp.float32),
        in_specs=[VMEM] * (len(described) + 2),
        out_specs=VMEM,
        scratch_shapes=[pltpu.VMEM((owners, FEATS, LANES), jnp.float32)],
        cost_estimate=cost(blocks, owners),
        name="far",
        compiler_params=pltpu.CompilerParams(vmem_limit_bytes=16 * MIB),
    )(*described, targets, near)


def image_kernel(root, arrived_ref, sketch_ref, image_ref, local_ref):
    total = arrived_ref[0]
    for k in range(1, arrived_ref.shape[0]):
        total = total + arrived_ref[k]
    image = total / root
    image_ref[...] = image
    image = in_order(image)
    first = image.astype(jnp.bfloat16)
    second = (image - first.astype(jnp.float32)).astype(jnp.bfloat16)
    both = jnp.concatenate([first, second], axis=0)
    over_lanes = (((1,), (1,)), ((), ()))
    for k in range(sketch_ref.shape[0] // (2 * LANES)):
        rows = sketch_ref[2 * k * LANES : 2 * (k + 1) * LANES, :]
        high = rows.astype(jnp.bfloat16)
        low = (rows - high.astype(jnp.float32)).astype(jnp.bfloat16)
        total = lax.dot_general(both, high, over_lanes, preferred_element_type=jnp.float32)
        total = total + lax.dot_general(both, low, over_lanes, preferred_element_type=jnp.float32)
        total = total[:SYSTEMS] + total[SYSTEMS:]
        for j in range(2):
            local_ref[:, 2 * k + j, :] = total[:, j * LANES : (j + 1) * LANES]


def image_and_sketch(arrived, sketch, root):
    rows = sketch.shape[0]
    return pl.pallas_call(
        functools.partial(image_kernel, root),
        out_shape=(
            jax.ShapeDtypeStruct((SYSTEMS, LANES), jnp.float32),
            jax.ShapeDtypeStruct((SYSTEMS, rows // LANES, LANES), jnp.float32),
        ),
        in_specs=[VMEM] * 2,
        out_specs=(VMEM,) * 2,
        name="image",
        compiler_params=pltpu.CompilerParams(vmem_limit_bytes=8 * MIB),
    )(arrived, sketch)


def sum_kernel(arrived_ref, out_ref):
    total = arrived_ref[0]
    for k in range(1, arrived_ref.shape[0]):
        total = total + arrived_ref[k]
    for k in range(out_ref.shape[0]):
        out_ref[k] = total


def sum_for_each(arrived, count):
    return pl.pallas_call(
        sum_kernel,
        out_shape=jax.ShapeDtypeStruct((count, *arrived.shape[1:]), jnp.float32),
        in_specs=[VMEM],
        out_specs=VMEM,
        name="addup",
        compiler_params=pltpu.CompilerParams(vmem_limit_bytes=4 * MIB),
    )(arrived)


def project_kernel(share, arrived_ref, basis_ref, out_ref):
    total = arrived_ref[0]
    for k in range(1, arrived_ref.shape[0]):
        total = total + arrived_ref[k]
    rows = total.shape[0] // share
    lane = lax.broadcasted_iota(jnp.int32, (1, LANES), 1)

    def whole(value):
        return jnp.sum(jnp.sum(value, axis=1, keepdims=True), axis=0, keepdims=True)

    lines, last = [], []
    for part in range(share):
        sketched = total[part * rows : (part + 1) * rows]
        basis = [basis_ref[j, part * rows : (part + 1) * rows, :] for j in range(KRYLOV)]
        scalars = jnp.zeros((1, LANES), jnp.float32)
        remainder = sketched
        for j in range(KRYLOV):
            coefficient = whole(basis[j] * sketched)
            scalars = jnp.where(lane == j, coefficient, scalars)
            remainder = remainder - coefficient * basis[j]
        norm = jnp.sqrt(whole(remainder * remainder) / (rows * LANES) + 1e-06)
        lines.append(remainder / norm)
        last.append(jnp.where(lane == KRYLOV, norm, scalars))
    message = jnp.concatenate(lines + last, axis=0)
    for k in range(out_ref.shape[0]):
        for j in range(message.shape[0]):
            out_ref[k, :, j * LANES : (j + 1) * LANES] = message[j : j + 1, :]


def project(arrived, basis, count):
    share = SYSTEMS // count
    return pl.pallas_call(
        functools.partial(project_kernel, share),
        out_shape=jax.ShapeDtypeStruct((count, 1, (arrived.shape[1] + share) * LANES), jnp.float32),
        in_specs=[VMEM] * 2,
        out_specs=VMEM,
        name="project",
        compiler_params=pltpu.CompilerParams(vmem_limit_bytes=4 * MIB),
    )(arrived, basis)


def finish_kernel(arrived_ref, image_ref, krylov_ref, next_ref, coefficients_ref, sketch_ref, norms_ref, lines):
    width, count = sketch_ref.shape[1], arrived_ref.shape[0]
    share = SYSTEMS // count
    for part in range(share):
        place = pl.ds(part, count, stride=share)
        for k in range(width // LANES):
            at = part * width + k * LANES
            lines[k, place, :] = arrived_ref[:, 0, at : at + LANES]
        at = share * width + part * LANES
        lines[width // LANES, place, :] = arrived_ref[:, 0, at : at + LANES]
    for k in range(width // LANES):
        sketch_ref[:, k * LANES : (k + 1) * LANES] = in_order(lines[k])
    scalars = in_order(lines[width // LANES])
    reduced = image_ref[...]
    for j in range(KRYLOV):
        reduced = reduced - scalars[:, j : j + 1] * krylov_ref[j]
    next_ref[...] = reduced / scalars[:, KRYLOV : KRYLOV + 1]
    across = jnp.transpose(scalars)
    coefficients_ref[...] = across[0:KRYLOV, :]
    norms_ref[...] = across[KRYLOV : KRYLOV + 1, :]


def finish(arrived, image, krylov):
    width = arrived.shape[2] * arrived.shape[0] // SYSTEMS - LANES
    return pl.pallas_call(
        finish_kernel,
        out_shape=(
            jax.ShapeDtypeStruct((SYSTEMS, LANES), jnp.float32),
            jax.ShapeDtypeStruct((KRYLOV, SYSTEMS), jnp.float32),
            jax.ShapeDtypeStruct((SYSTEMS, width), jnp.float32),
            jax.ShapeDtypeStruct((1, SYSTEMS), jnp.float32),
        ),
        in_specs=[VMEM] * 3,
        out_specs=(VMEM,) * 4,
        scratch_shapes=[pltpu.VMEM((width // LANES + 1, SYSTEMS, LANES), jnp.float32)],
        name="finish",
        compiler_params=pltpu.CompilerParams(vmem_limit_bytes=8 * MIB),
    )(arrived, image, krylov)


def step(points, labels, shape_scale, krylov_basis, sketch, sketched_basis):
    everything = lax.axis_size(ALL) * points.shape[1]
    system = jnp.bitwise_xor(lax.axis_index(OWNERS), 2 * lax.axis_index(Y1))
    share = SYSTEMS // lax.axis_size(OWNERS)
    basis = lax.dynamic_slice_in_dim(sketched_basis, system * share, share, axis=1)
    basis = basis.reshape(KRYLOV, -1, LANES)
    sources, targets = messages(points, labels, shape_scale, krylov_basis, lax.axis_size(ROW))
    all_sources = exchange(sources, ROW)
    near = with_other(targets, COLUMN[2])
    near = with_other(near, COLUMN[1])
    far = lax.ppermute(near, (Z2, Z1), ((0, 3), (1, 2), (2, 1), (3, 0)))
    near, all_sources, basis = lax.optimization_barrier((near, all_sources, basis))
    other_sources = swap(all_sources, CORE)
    partial_value, *first = near_product(all_sources, near)
    partial_value, *second = near_product(other_sources, near, partial_value)
    partial_value = far_product((*first, *second), far, partial_value)
    image, local_sketch = image_and_sketch(
        exchange(partial_value, COLUMN), sketch, math.sqrt(everything)
    )
    local_sketch = local_sketch.reshape(lax.axis_size(OWNERS), -1, LANES)
    over_owners = sum_for_each(exchange(local_sketch, OWNERS), len(PAIRS[0]))
    message = project(exchange_layers(over_owners), basis, lax.axis_size(OWNERS))
    next_vector, coefficients, sketch_next, norms = finish(
        exchange(message, OWNERS), image, krylov_basis
    )
    return (next_vector, coefficients, sketch_next, norms.reshape(-1))


def solution(mesh):
    torus = Mesh(mesh.devices.reshape((2,) * len(ALL)), ALL)
    in_specs = (P(None, ALL), P(ALL), P(ALL), P(None, None, ALL), P(None, ALL), P())
    out_specs = (P(None, ALL), P(), P(), P())
    return jax.shard_map(step, mesh=torus, in_specs=in_specs, out_specs=out_specs, check_vma=False)
```

```python
import functools
import math

import jax
import jax.numpy as jnp
from jax import lax
from jax.experimental import pallas as pl
from jax.experimental.pallas import tpu as pltpu
from jax.sharding import Mesh
from jax.sharding import PartitionSpec as P

SYSTEMS = 32
KRYLOV = 8
FEATS = 32
LANES = 128
X1, X0, Z2, Z1, Z0, Y1, Y0, CORE = ALL = ("x1", "x0", "z2", "z1", "z0", "y1", "y0", "core")
COLUMN = (Z2, Z1, Z0)
NEAR = (0, 2, 1, 3)
ROW = (X1, X0, Y1, Y0)
OWNERS = (X1, X0, Y0, CORE)
LAYERS = (Y1, Y0, Z2, Z1, Z0)
PAIRS = tuple(tuple(8 * y + z for y in pair for z in range(8)) for pair in ((0, 3), (1, 2)))
VMEM = pl.BlockSpec(memory_space=pltpu.VMEM)
MIB = 2**20


def exchange(value, axis):
    return lax.all_to_all(value, axis, 0, 0, tiled=True)


def exchange_layers(value):
    return lax.all_to_all(value, LAYERS, 0, 0, axis_index_groups=PAIRS, tiled=True)


def in_order(value):
    rows = value.shape[0]
    swapped = jnp.concatenate([value[k ^ 4 : (k ^ 4) + 4] for k in range(0, rows, 4)], axis=0)
    return jnp.where(lax.axis_index(Y1) == 1, swapped, value)


def swap(value, axis):
    return lax.ppermute(value, axis, ((0, 1), (1, 0)))


def with_other(value, axis):
    return jnp.concatenate([value, swap(value, axis)], axis=0)


def parts(value):
    first = value.astype(jnp.bfloat16).astype(jnp.float32)
    rest = value - first
    second = rest.astype(jnp.bfloat16).astype(jnp.float32)
    return [first, second, rest - second]


def wide(tiles):
    return jnp.concatenate(tiles, axis=1)


def message_kernel(points_ref, labels_ref, scale_ref, krylov_ref, sources_ref, targets_ref, vector, row, copied, sem):
    taken = [
        pltpu.make_async_copy(krylov_ref.at[krylov_ref.shape[0] - 1], vector, sem.at[0]),
        pltpu.make_async_copy(points_ref, row.at[0:3], sem.at[1]),
        pltpu.make_async_copy(scale_ref, row.at[3:4], sem.at[2]),
        pltpu.make_async_copy(labels_ref, copied, sem.at[3]),
    ]
    for copy in taken:
        copy.start()
    for copy in taken:
        copy.wait()
    for k in range(sources_ref.shape[0]):
        sources_ref[k, 0:SYSTEMS, :] = vector[...]
        sources_ref[k, SYSTEMS : SYSTEMS + 4, :] = row[...]
    targets_ref[0, 0:3, :] = row[0:3, :]
    targets_ref[0, 3:4, :] = copied[...].astype(jnp.float32)


def messages(points, labels, shape_scale, krylov, count):
    hbm = pl.BlockSpec(memory_space=pltpu.HBM)
    return pl.pallas_call(
        message_kernel,
        out_shape=(
            jax.ShapeDtypeStruct((count, SYSTEMS + 4, LANES), jnp.float32),
            jax.ShapeDtypeStruct((1, 4, LANES), jnp.float32),
        ),
        in_specs=[hbm] * 4,
        out_specs=(VMEM,) * 2,
        scratch_shapes=[
            pltpu.VMEM((SYSTEMS, LANES), jnp.float32),
            pltpu.VMEM((4, LANES), jnp.float32),
            pltpu.VMEM((1, LANES), jnp.int32),
            pltpu.SemaphoreType.DMA((4,)),
        ],
        name="messages",
    )(points, labels[None, :], shape_scale[None, :], krylov)


def stored(rows, out_ref):
    zero = jnp.zeros(rows[0].shape, jnp.float32)
    for k, value in enumerate(rows + [zero] * (FEATS - len(rows))):
        out_ref[:, k, :] = value


def pair_of(ref, step):
    return wide([ref[2 * step], ref[2 * step + 1]])


def describe_sources(source_ref, feats_ref, weights_ref):
    coords = [source_ref[:, SYSTEMS + a, :] - 0.5 for a in range(3)]
    scale = source_ref[:, SYSTEMS + 3, :]
    per_square = 1.0 / (scale * scale)
    rows = []
    for value in [c * per_square for c in coords] + [per_square]:
        a, b, c = parts(value)
        rows += [a, a, b, b, a, c]
    square = coords[0] * coords[0] + coords[1] * coords[1] + coords[2] * coords[2]
    stored(rows + parts(square * per_square + 1.0), feats_ref)
    for step in range(weights_ref.shape[0]):
        weight = wide([source_ref[2 * step + j, 0:SYSTEMS, :] for j in range(2)])
        scale = wide([source_ref[2 * step + j, SYSTEMS + 3 : SYSTEMS + 4, :] for j in range(2)])
        terms = []
        for value in (weight / scale, weight * scale):
            first = value.astype(jnp.bfloat16)
            terms += [first, (value - first.astype(jnp.float32)).astype(jnp.bfloat16)]
        weights_ref[step] = jnp.concatenate(terms, axis=0)


def describe_targets(target_ref, feats_ref):
    coords = [target_ref[:, a, :] - 0.5 for a in range(3)]
    square = coords[0] * coords[0] + coords[1] * coords[1] + coords[2] * coords[2]
    rows = []
    for value in [-2.0 * c for c in coords] + [square]:
        a, b, c = parts(value)
        rows += [a, b, a, b, c, a]
    stored(rows + [jnp.ones(square.shape, jnp.float32)] * 3, feats_ref)


def products(sources, target_ref, target_feats):
    indices = range(target_ref.shape[0] // 2)
    feats = [pair_of(target_feats, index).astype(jnp.bfloat16) for index in indices]
    inner = [wide([target_ref[2 * index + j, 3:4, :] for j in range(2)]) > 0.5 for index in indices]
    totals = [jnp.zeros((4 * SYSTEMS, 2 * LANES), jnp.float32) for index in indices]
    for source_feats, weights in sources:
        for step in range(weights.shape[0]):
            source = pair_of(source_feats, step).astype(jnp.bfloat16)
            weight = weights[step]
            for index in indices:
                ratio = lax.dot_general(
                    source, feats[index], (((0,), (0,)), ((), ())), preferred_element_type=jnp.float32
                )
                root = lax.rsqrt(ratio)
                kernel = root * jnp.where(inner[index], 2.0 + root * root, ratio)
                first = kernel.astype(jnp.bfloat16)
                second = (kernel - first.astype(jnp.float32)).astype(jnp.bfloat16)
                totals[index] = (
                    totals[index]
                    + jnp.dot(weight, first, preferred_element_type=jnp.float32)
                    + jnp.dot(weight, second, preferred_element_type=jnp.float32)
                )
    results = []
    for index in indices:
        a, b, c, d = (totals[index][k * SYSTEMS : (k + 1) * SYSTEMS] for k in range(4))
        result = jnp.where(inner[index], a + b, c + d)
        results += [result[:, :LANES], result[:, LANES:]]
    return results


def near_kernel(*refs):
    (source_ref, target_ref, *before, out_ref, source_feats, weights, target_feats) = refs
    describe_sources(source_ref, source_feats, weights)
    describe_targets(target_ref, target_feats)
    for k, part in enumerate(products([(source_feats, weights)], target_ref, target_feats)):
        out_ref[k] = part + before[0][k] if before else part


def far_kernel(first_feats, first_weights, second_feats, second_weights, target_ref, near_ref, out_ref, target_feats):
    describe_targets(target_ref, target_feats)
    place = lax.axis_index(COLUMN)
    near = near_ref.shape[0]
    for k in range(near):
        out_ref[jnp.bitwise_xor(place, NEAR[k])] = near_ref[k]
    sources = [(first_feats, first_weights), (second_feats, second_weights)]
    for k, part in enumerate(products(sources, target_ref, target_feats)):
        out_ref[jnp.bitwise_xor(place, 6 ^ NEAR[k])] = part


def cost(sources, targets):
    pairs = sources * targets * LANES * LANES
    return pl.CostEstimate(flops=12 * SYSTEMS * pairs, bytes_accessed=2**20, transcendentals=pairs)


def near_product(sources, targets, *before):
    blocks, owners = sources.shape[0], targets.shape[0]
    return pl.pallas_call(
        near_kernel,
        out_shape=(
            jax.ShapeDtypeStruct((owners, SYSTEMS, LANES), jnp.float32),
            jax.ShapeDtypeStruct((blocks, FEATS, LANES), jnp.float32),
            jax.ShapeDtypeStruct((blocks // 2, 4 * SYSTEMS, 2 * LANES), jnp.bfloat16),
        ),
        in_specs=[VMEM] * (2 + len(before)),
        out_specs=(VMEM,) * 3,
        scratch_shapes=[pltpu.VMEM((owners, FEATS, LANES), jnp.float32)],
        cost_estimate=cost(blocks, owners),
        name="near",
        compiler_params=pltpu.CompilerParams(vmem_limit_bytes=16 * MIB),
    )(sources, targets, *before)


def far_product(described, targets, near):
    blocks, owners = sum(feats.shape[0] for feats in described[::2]), targets.shape[0]
    return pl.pallas_call(
        far_kernel,
        out_shape=jax.ShapeDtypeStruct((owners + near.shape[0], SYSTEMS, LANES), jnp.float32),
        in_specs=[VMEM] * (len(described) + 2),
        out_specs=VMEM,
        scratch_shapes=[pltpu.VMEM((owners, FEATS, LANES), jnp.float32)],
        cost_estimate=cost(blocks, owners),
        name="far",
        compiler_params=pltpu.CompilerParams(vmem_limit_bytes=16 * MIB),
    )(*described, targets, near)


def image_kernel(root, arrived_ref, sketch_ref, image_ref, local_ref):
    total = arrived_ref[0]
    for k in range(1, arrived_ref.shape[0]):
        total = total + arrived_ref[k]
    image = total / root
    image_ref[...] = image
    image = in_order(image)
    first = image.astype(jnp.bfloat16)
    second = (image - first.astype(jnp.float32)).astype(jnp.bfloat16)
    both = jnp.concatenate([first, second], axis=0)
    over_lanes = (((1,), (1,)), ((), ()))
    for k in range(sketch_ref.shape[0] // (2 * LANES)):
        rows = sketch_ref[2 * k * LANES : 2 * (k + 1) * LANES, :]
        high = rows.astype(jnp.bfloat16)
        low = (rows - high.astype(jnp.float32)).astype(jnp.bfloat16)
        total = lax.dot_general(both, high, over_lanes, preferred_element_type=jnp.float32)
        total = total + lax.dot_general(both, low, over_lanes, preferred_element_type=jnp.float32)
        total = total[:SYSTEMS] + total[SYSTEMS:]
        for j in range(2):
            local_ref[:, 2 * k + j, :] = total[:, j * LANES : (j + 1) * LANES]


def image_and_sketch(arrived, sketch, root):
    rows = sketch.shape[0]
    return pl.pallas_call(
        functools.partial(image_kernel, root),
        out_shape=(
            jax.ShapeDtypeStruct((SYSTEMS, LANES), jnp.float32),
            jax.ShapeDtypeStruct((SYSTEMS, rows // LANES, LANES), jnp.float32),
        ),
        in_specs=[VMEM] * 2,
        out_specs=(VMEM,) * 2,
        name="image",
        compiler_params=pltpu.CompilerParams(vmem_limit_bytes=8 * MIB),
    )(arrived, sketch)


def sum_kernel(arrived_ref, out_ref):
    total = arrived_ref[0]
    for k in range(1, arrived_ref.shape[0]):
        total = total + arrived_ref[k]
    for k in range(out_ref.shape[0]):
        out_ref[k] = total


def sum_for_each(arrived, count):
    return pl.pallas_call(
        sum_kernel,
        out_shape=jax.ShapeDtypeStruct((count, *arrived.shape[1:]), jnp.float32),
        in_specs=[VMEM],
        out_specs=VMEM,
        name="addup",
        compiler_params=pltpu.CompilerParams(vmem_limit_bytes=4 * MIB),
    )(arrived)


def project_kernel(share, arrived_ref, basis_ref, out_ref):
    total = arrived_ref[0]
    for k in range(1, arrived_ref.shape[0]):
        total = total + arrived_ref[k]
    rows = total.shape[0] // share
    lane = lax.broadcasted_iota(jnp.int32, (1, LANES), 1)

    def whole(value):
        return jnp.sum(jnp.sum(value, axis=1, keepdims=True), axis=0, keepdims=True)

    lines, last = [], []
    for part in range(share):
        sketched = total[part * rows : (part + 1) * rows]
        basis = [basis_ref[j, part * rows : (part + 1) * rows, :] for j in range(KRYLOV)]
        scalars = jnp.zeros((1, LANES), jnp.float32)
        remainder = sketched
        for j in range(KRYLOV):
            coefficient = whole(basis[j] * sketched)
            scalars = jnp.where(lane == j, coefficient, scalars)
            remainder = remainder - coefficient * basis[j]
        norm = jnp.sqrt(whole(remainder * remainder) / (rows * LANES) + 1e-06)
        lines.append(remainder / norm)
        last.append(jnp.where(lane == KRYLOV, norm, scalars))
    message = jnp.concatenate(lines + last, axis=0)
    for k in range(out_ref.shape[0]):
        for j in range(message.shape[0]):
            out_ref[k, :, j * LANES : (j + 1) * LANES] = message[j : j + 1, :]


def project(arrived, basis, count):
    share = SYSTEMS // count
    return pl.pallas_call(
        functools.partial(project_kernel, share),
        out_shape=jax.ShapeDtypeStruct((count, 1, (arrived.shape[1] + share) * LANES), jnp.float32),
        in_specs=[VMEM] * 2,
        out_specs=VMEM,
        name="project",
        compiler_params=pltpu.CompilerParams(vmem_limit_bytes=4 * MIB),
    )(arrived, basis)


def finish_kernel(arrived_ref, image_ref, krylov_ref, next_ref, coefficients_ref, sketch_ref, norms_ref, lines):
    width, count = sketch_ref.shape[1], arrived_ref.shape[0]
    share = SYSTEMS // count
    for part in range(share):
        place = pl.ds(part, count, stride=share)
        for k in range(width // LANES):
            at = part * width + k * LANES
            lines[k, place, :] = arrived_ref[:, 0, at : at + LANES]
        at = share * width + part * LANES
        lines[width // LANES, place, :] = arrived_ref[:, 0, at : at + LANES]
    for k in range(width // LANES):
        sketch_ref[:, k * LANES : (k + 1) * LANES] = in_order(lines[k])
    scalars = in_order(lines[width // LANES])
    reduced = image_ref[...]
    for j in range(KRYLOV):
        reduced = reduced - scalars[:, j : j + 1] * krylov_ref[j]
    next_ref[...] = reduced / scalars[:, KRYLOV : KRYLOV + 1]
    across = jnp.transpose(scalars)
    coefficients_ref[...] = across[0:KRYLOV, :]
    norms_ref[...] = across[KRYLOV : KRYLOV + 1, :]


def finish(arrived, image, krylov):
    width = arrived.shape[2] * arrived.shape[0] // SYSTEMS - LANES
    return pl.pallas_call(
        finish_kernel,
        out_shape=(
            jax.ShapeDtypeStruct((SYSTEMS, LANES), jnp.float32),
            jax.ShapeDtypeStruct((KRYLOV, SYSTEMS), jnp.float32),
            jax.ShapeDtypeStruct((SYSTEMS, width), jnp.float32),
            jax.ShapeDtypeStruct((1, SYSTEMS), jnp.float32),
        ),
        in_specs=[VMEM] * 3,
        out_specs=(VMEM,) * 4,
        scratch_shapes=[pltpu.VMEM((width // LANES + 1, SYSTEMS, LANES), jnp.float32)],
        name="finish",
        compiler_params=pltpu.CompilerParams(vmem_limit_bytes=8 * MIB),
    )(arrived, image, krylov)


def step(points, labels, shape_scale, krylov_basis, sketch, sketched_basis):
    everything = lax.axis_size(ALL) * points.shape[1]
    system = jnp.bitwise_xor(lax.axis_index(OWNERS), 2 * lax.axis_index(Y1))
    share = SYSTEMS // lax.axis_size(OWNERS)
    basis = lax.dynamic_slice_in_dim(sketched_basis, system * share, share, axis=1)
    basis = basis.reshape(KRYLOV, -1, LANES)
    sources, targets = messages(points, labels, shape_scale, krylov_basis, lax.axis_size(ROW))
    all_sources = exchange(sources, ROW)
    near = with_other(targets, Z1)
    near = with_other(near, Z0)
    far = lax.ppermute(near, (Z2, Z1), ((0, 3), (1, 2), (2, 1), (3, 0)))
    near, all_sources, basis = lax.optimization_barrier((near, all_sources, basis))
    other_sources = swap(all_sources, CORE)
    partial_value, *first = near_product(all_sources, near)
    partial_value, *second = near_product(other_sources, near, partial_value)
    partial_value = far_product((*first, *second), far, partial_value)
    image, local_sketch = image_and_sketch(
        exchange(partial_value, COLUMN), sketch, math.sqrt(everything)
    )
    local_sketch = local_sketch.reshape(lax.axis_size(OWNERS), -1, LANES)
    over_owners = sum_for_each(exchange(local_sketch, OWNERS), len(PAIRS[0]))
    message = project(exchange_layers(over_owners), basis, lax.axis_size(OWNERS))
    next_vector, coefficients, sketch_next, norms = finish(
        exchange(message, OWNERS), image, krylov_basis
    )
    return (next_vector, coefficients, sketch_next, norms.reshape(-1))


def solution(mesh):
    torus = Mesh(mesh.devices.reshape((2,) * len(ALL)), ALL)
    in_specs = (P(None, ALL), P(ALL), P(ALL), P(None, None, ALL), P(None, ALL), P())
    out_specs = (P(None, ALL), P(), P(), P())
    return jax.shard_map(step, mesh=torus, in_specs=in_specs, out_specs=out_specs, check_vma=False)
```
